32 devices in a mesh: dp: 4 (over y, x), ctx: 8 (over z, core).
Axes of the slice: x: 2, y: 2, z: 4, core: 2. Of those that a mesh axis runs over, the one named last changes fastest.
Arguments:
- query: bfloat16 [4, 1024, 4096], P('dp', 'ctx'), may hold values from -6 to 6
- key: bfloat16 [4, 1024, 256], P('dp', 'ctx'), may hold values from -6 to 6
- value: bfloat16 [4, 1024, 256], P('dp', 'ctx'), may hold values from -6 to 6
- span_order: int32 [4, 16], P('dp'), may hold values from 0 to 15, each once within a row
- expert_ids: int32 [4, 1024, 8], P('dp', 'ctx'), may hold values from 0 to 127, as said below
- expert_gates: float32 [4, 1024, 8], P('dp', 'ctx'), may hold values from 0.02 to 0.2
- trainable: int32 [8], replicated, may hold values from 0 to 127, as said below
- norm_gain: float32 [4096], replicated, may hold values from 0.5 to 1.5
- upstream: bfloat16 [4, 1024, 4096], P('dp', 'ctx'), may hold values from -6 to 6
- expert_weights: bfloat16 [8, 768, 3, 4096], P('ctx'), may hold values from -0.09375 to 0.09375
Outputs:
- d_query: bfloat16 [4, 1024, 4096], P('dp', 'ctx')
- key_gradient: bfloat16 [4, 1024, 256], P('dp', 'ctx')
- value_gradient: bfloat16 [4, 1024, 256], P('dp', 'ctx')
- expert_grads: bfloat16 [8, 768, 3, 4096], P('ctx', 'dp')
The draws below stay inside these ranges and needn't reach their ends.
Inputs may be any that keep to these rules, and one draw needn't show every extreme that they name: `span_order`: each row is a permutation of the 16 span numbers. `expert_ids`: the 8 numbers of a token are distinct; among the 128 rows of one device (aligned blocks of 128 rows of a document) at most 12 name the same expert. `trainable`: distinct expert numbers.
All inputs are finite; a program needn't handle non-finite values.
Results may differ from the reference program's by a relative error of at most 0.02.
Values may be sent and summed in bfloat16 or wider, within the bound.
No kernel may reach another device: no remote copies, remote signals or barrier semaphores. Data moves between devices by JAX's collectives and lax.ppermute only.
A program may use at most 128 MiB of HBM per device.

```python
import math
import jax
import jax.numpy as jnp
from jax import lax

D = 4096
QUERY_HEADS = 32
KEY_VALUE_HEADS = 2
HEAD_SIZE = 128
H = 768
EXPERTS = 128
TOP = 8
TOK_DEV = 128
TRAIN = 8
DOCUMENT_LENGTH = 1024
CAP = 12
N_DP = 4
N_CTX = 8


def drawn_fields(base_key):
    seed_all = jax.random.fold_in(base_key, 11)
    key_query, key_random_keys = jax.random.split(seed_all, 2)
    query_vals = jnp.clip(jax.random.normal(key_query, (N_DP, DOCUMENT_LENGTH, QUERY_HEADS * HEAD_SIZE), jnp.float32), -5.5, 5.5)
    key_entries = jnp.clip(jax.random.normal(key_random_keys, (N_DP, DOCUMENT_LENGTH, KEY_VALUE_HEADS * HEAD_SIZE), jnp.float32), -5.5, 5.5)
    return (query_vals, key_entries)


def routing_tables(base_key):
    seed_all = jax.random.fold_in(base_key, 29)
    key_pick, key_full, key_level, key_noise, key_row_block = jax.random.split(seed_all, 5)
    trainable = jax.random.permutation(key_pick, EXPERTS)[:TRAIN].astype(jnp.int32)
    full_slot = jax.random.randint(key_full, (), 0, TRAIN)
    full_expert = jnp.sum(jnp.where(jnp.arange(TRAIN) == full_slot, trainable, 0))
    expert_num = jnp.arange(EXPERTS, dtype=jnp.int32)
    levels = jax.random.randint(key_level, (EXPERTS,), 0, 4)
    levels = jnp.where(expert_num == full_expert, 8, levels)
    block_count = N_DP * N_CTX
    entries = EXPERTS * CAP
    entry_num = jnp.arange(entries, dtype=jnp.int32)
    owner_of = entry_num // CAP
    noise_vals = jax.random.randint(key_noise, (block_count, entries), 0, 4096)
    priority = (levels[owner_of][None, :] * 4096 + noise_vals) * entries + entry_num[None, :]
    assigned = TOK_DEV * TOP
    kept_idx = jnp.sort(jnp.argsort(-priority, axis=1)[:, :assigned], axis=1)
    chosen = (kept_idx // CAP).astype(jnp.int32)
    id_table = chosen.reshape(block_count, TOP, TOK_DEV).transpose(0, 2, 1)
    shuffle = jax.random.randint(key_row_block, (block_count, TOK_DEV), 0, 4096) * TOK_DEV + jnp.arange(TOK_DEV)[None, :]
    row_perm = jnp.argsort(shuffle, axis=1)
    id_table = jnp.take_along_axis(id_table, row_perm[:, :, None], axis=1)
    return (trainable, id_table.reshape(N_DP, DOCUMENT_LENGTH, TOP).astype(jnp.int32))


def draw_query(key, part):
    return drawn_fields(key)[0].astype(jnp.bfloat16)


def draw_key(key, part):
    return drawn_fields(key)[1].astype(jnp.bfloat16)


def draw_expert_ids(key, part):
    return routing_tables(key)[1]


def draw_trainable(key, part):
    return routing_tables(key)[0]


def steps_of(rng, shape, cuts, low, high):
    def one(dim, blocks):
        steps = jax.random.uniform(jax.random.fold_in(jax.random.fold_in(rng, 6), dim), (blocks,), jnp.float32, low / len(cuts), high / len(cuts))
        return jnp.repeat(jnp.exp(steps), shape[dim] // blocks).reshape((-1,) + (1,) * (len(shape) - dim - 1))

    loudness = one(*cuts[0])
    for cut in cuts[1:]:
        loudness = loudness * one(*cut)
    return loudness


def gaussian(own_key, dims, deviation, reach, cuts=(), held_as=jnp.bfloat16):
    values = deviation * jax.random.normal(own_key, dims, jnp.float32)
    if cuts:
        values = values * steps_of(own_key, dims, cuts, -0.22, 0.18)
    return jnp.clip(values, -reach, reach).astype(held_as)


def setup_inputs(seed: int = 0) -> dict:
    arg_keys = jax.random.split(jax.random.key(seed), 11)
    return {
        "query": draw_query(jax.random.fold_in(arg_keys[10], 71), 0),
        "key": draw_key(jax.random.fold_in(arg_keys[10], 71), 0),
        "value": gaussian(arg_keys[2], (N_DP, DOCUMENT_LENGTH, KEY_VALUE_HEADS * HEAD_SIZE), 1.0, 6.0, ((0, 4), (1, 8))),
        "span_order": jax.vmap(lambda own: jax.random.permutation(own, 2 * N_CTX))(jax.random.split(arg_keys[3], N_DP)).reshape((N_DP, 2 * N_CTX)).astype(jnp.int32),
        "expert_ids": draw_expert_ids(jax.random.fold_in(arg_keys[10], 71), 0),
        "expert_gates": jnp.clip(jnp.exp(math.log(0.2) - 2.3025851 * jax.random.uniform(arg_keys[5], (N_DP, DOCUMENT_LENGTH, TOP), jnp.float32) ** steps_of(arg_keys[5], (N_DP, DOCUMENT_LENGTH, TOP), ((0, 4), (1, 8)), -0.2, 0.2)), 0.02, 0.2),
        "trainable": draw_trainable(jax.random.fold_in(arg_keys[10], 71), 0),
        "norm_gain": jnp.clip(1.0 + 0.1 * jax.random.normal(arg_keys[7], (D,), jnp.float32), 0.5, 1.5),
        "upstream": gaussian(arg_keys[8], (N_DP, DOCUMENT_LENGTH, D), 1.0, 6.0, ((0, 4), (1, 8))),
        "expert_weights": gaussian(arg_keys[9], (TRAIN, H, 3, D), D ** -0.5, 0.09375, ((0, 8),)),
    }


MASK_FILLER = -1e+30
EPSILON = 1e-06

def positions(span_seq):
    row_index = jnp.arange(DOCUMENT_LENGTH, dtype=jnp.int32)
    half_rows = TOK_DEV // 2
    return span_seq[row_index // half_rows] * half_rows + row_index % half_rows

def head_scores(query_head, key_head, visible):
    raw_scores = jnp.dot(query_head, key_head.T, preferred_element_type=jnp.float32) * HEAD_SIZE ** (-0.5)
    return jnp.where(visible, raw_scores, MASK_FILLER)

def document_grads(query, key, value, span_seq, routes_now, gate_vals, trainable, norm_gain, upstream, expert_weights):
    heads_per_group = QUERY_HEADS // KEY_VALUE_HEADS
    place_now = positions(span_seq)
    visible = place_now[None, :] <= place_now[:, None]
    query_heads = query.reshape(DOCUMENT_LENGTH, QUERY_HEADS, HEAD_SIZE).transpose(1, 0, 2)
    key_head_rows = key.reshape(DOCUMENT_LENGTH, KEY_VALUE_HEADS, HEAD_SIZE).transpose(1, 0, 2)
    value_head_rows = value.reshape(DOCUMENT_LENGTH, KEY_VALUE_HEADS, HEAD_SIZE).transpose(1, 0, 2)
    head_number = jnp.arange(QUERY_HEADS, dtype=jnp.int32)

    def forward(item_now):
        query_head, number = item_now
        key_head = key_head_rows[number // heads_per_group]
        value_head = value_head_rows[number // heads_per_group]
        raw_scores = head_scores(query_head, key_head, visible)
        peak = lax.optimization_barrier(jnp.max(raw_scores, axis=1))
        spread = peak + jnp.log(lax.optimization_barrier(jnp.sum(jnp.exp(raw_scores - peak[:, None]), axis=1)))
        weights = jnp.where(visible, jnp.exp(raw_scores - spread[:, None]), 0.0).astype(jnp.bfloat16)
        output = jnp.dot(weights, value_head, preferred_element_type=jnp.float32).astype(jnp.bfloat16)
        return (output, spread)
    outputs, spreads = lax.map(forward, (query_heads, head_number))
    mixed_rows = outputs.transpose(1, 0, 2).reshape(DOCUMENT_LENGTH, D)
    features = mixed_rows.astype(jnp.float32)
    factor = lax.rsqrt(lax.optimization_barrier(jnp.mean(features * features, axis=1, keepdims=True)) + EPSILON)
    normed = (features * factor * norm_gain[None, :]).astype(jnp.bfloat16)
    most_rows = N_CTX * CAP

    def expert(item_now):
        expert_num, weights = item_now
        is_match = routes_now == expert_num
        chosen = jnp.any(is_match, axis=1)
        row_gate = lax.optimization_barrier(jnp.sum(jnp.where(is_match, gate_vals, 0.0), axis=1))
        picked = jnp.nonzero(chosen, size=most_rows, fill_value=0)[0].astype(jnp.int32)
        valid = jnp.arange(most_rows, dtype=jnp.int32) < jnp.sum(chosen.astype(jnp.int32))
        routed = jnp.where(valid[:, None], normed[picked], jnp.zeros((), jnp.bfloat16))
        weighted = jnp.where(valid[:, None], row_gate[picked][:, None] * upstream[picked].astype(jnp.float32), 0.0).astype(jnp.bfloat16)
        w_gate = weights[:, 0, :]
        w_up = weights[:, 1, :]
        w_down = weights[:, 2, :]
        gate_in = jnp.dot(routed, w_gate.T, preferred_element_type=jnp.float32)
        up_in = jnp.dot(routed, w_up.T, preferred_element_type=jnp.float32)
        back_grad = jnp.dot(weighted, w_down.T, preferred_element_type=jnp.float32)
        activated = jax.nn.silu(gate_in)
        product = (activated * up_in).astype(jnp.bfloat16)
        sigma = jax.nn.sigmoid(gate_in)
        grad_gate = (back_grad * up_in * sigma * (1.0 + gate_in * (1.0 - sigma))).astype(jnp.bfloat16)
        grad_up = (back_grad * activated).astype(jnp.bfloat16)
        returned = (jnp.dot(grad_gate, w_gate, preferred_element_type=jnp.float32) + jnp.dot(grad_up, w_up, preferred_element_type=jnp.float32)).astype(jnp.bfloat16)
        partial_sum = jnp.stack([jnp.dot(grad_gate.T, routed, preferred_element_type=jnp.float32), jnp.dot(grad_up.T, routed, preferred_element_type=jnp.float32), jnp.dot(product.T, weighted, preferred_element_type=jnp.float32)], axis=1)
        return (partial_sum, returned, picked, valid)
    partials, returned, picked, valid = lax.map(expert, (trainable, expert_weights))
    contrib = jnp.where(valid.reshape(-1)[:, None], returned.reshape(-1, D).astype(jnp.float32), 0.0)
    input_grad = jnp.zeros((DOCUMENT_LENGTH, D), jnp.float32).at[picked.reshape(-1)].add(contrib)
    gradnorm = norm_gain[None, :] * input_grad
    into_norm = factor * gradnorm - features * (factor * factor * factor) * lax.optimization_barrier(jnp.mean(gradnorm * features, axis=1, keepdims=True))
    grad_mixed = (upstream.astype(jnp.float32) + into_norm).astype(jnp.bfloat16)
    grad_heads = grad_mixed.reshape(DOCUMENT_LENGTH, QUERY_HEADS, HEAD_SIZE).transpose(1, 0, 2)

    def backward(item_now):
        query_head, out_head, grad_head, spread, number = item_now
        key_head = key_head_rows[number // heads_per_group]
        value_head = value_head_rows[number // heads_per_group]
        raw_scores = head_scores(query_head, key_head, visible)
        prob_full = jnp.where(visible, jnp.exp(raw_scores - spread[:, None]), 0.0)
        delta_sum = lax.optimization_barrier(jnp.sum(grad_head.astype(jnp.float32) * out_head.astype(jnp.float32), axis=1))
        pushed = jnp.dot(grad_head, value_head.T, preferred_element_type=jnp.float32)
        slopes = (prob_full * (pushed - delta_sum[:, None])).astype(jnp.bfloat16)
        inv_root = HEAD_SIZE ** (-0.5)
        query_grad = jnp.dot(slopes, key_head, preferred_element_type=jnp.float32) * inv_root
        key_grad = jnp.dot(slopes.T, query_head, preferred_element_type=jnp.float32) * inv_root
        value_grad = jnp.dot(prob_full.astype(jnp.bfloat16).T, grad_head, preferred_element_type=jnp.float32)
        return (query_grad, key_grad, value_grad)
    query_grads, key_gradient_list, value_gradient_list = lax.map(backward, (query_heads, outputs, grad_heads, spreads, head_number))
    d_query = query_grads.astype(jnp.bfloat16).transpose(1, 0, 2).reshape(DOCUMENT_LENGTH, QUERY_HEADS * HEAD_SIZE)
    key_gradient = lax.optimization_barrier(jnp.sum(key_gradient_list.reshape(KEY_VALUE_HEADS, heads_per_group, DOCUMENT_LENGTH, HEAD_SIZE), axis=1)).astype(jnp.bfloat16).transpose(1, 0, 2).reshape(DOCUMENT_LENGTH, KEY_VALUE_HEADS * HEAD_SIZE)
    value_gradient = lax.optimization_barrier(jnp.sum(value_gradient_list.reshape(KEY_VALUE_HEADS, heads_per_group, DOCUMENT_LENGTH, HEAD_SIZE), axis=1)).astype(jnp.bfloat16).transpose(1, 0, 2).reshape(DOCUMENT_LENGTH, KEY_VALUE_HEADS * HEAD_SIZE)
    return (d_query, key_gradient, value_gradient, partials)

def reference(query, key, value, span_order, expert_ids, expert_gates, trainable, norm_gain, upstream, expert_weights):
    query_list = []
    key_list = []
    value_list = []
    total_sum = jnp.zeros((TRAIN, H, 3, D), jnp.float32)
    for sequence in range(N_DP):
        d_query, key_gradient, value_gradient, partials = document_grads(query[sequence], key[sequence], value[sequence], span_order[sequence], expert_ids[sequence], expert_gates[sequence], trainable, norm_gain, upstream[sequence], expert_weights)
        query_list.append(d_query)
        key_list.append(key_gradient)
        value_list.append(value_gradient)
        total_sum = total_sum + lax.optimization_barrier(partials.astype(jnp.bfloat16)).astype(jnp.float32)
    return (jnp.stack(query_list), jnp.stack(key_list), jnp.stack(value_list), total_sum.astype(jnp.bfloat16))
```

```python
import math

import jax
import jax.numpy as jnp
from jax import lax
from jax.experimental import pallas as pl
from jax.experimental.pallas import tpu as pltpu
from jax.sharding import PartitionSpec as P

HEADS_PER_GROUP = 16
HEAD_SIZE = 128
CAP = 12
EPSILON = 1e-06
MASK_FILLER = -1e30
SCALE = HEAD_SIZE ** (-0.5)
LOG2E = 1.4426950408889634
FOLD = 2
PIECE = FOLD * CAP
STEP_HEADS = 4
F32 = jnp.float32
BF16 = jnp.bfloat16


def mm(a, b):
    return lax.dot_general(a, b, (((1,), (0,)), ((), ())), preferred_element_type=F32)


def mm_t(a, b):
    return lax.dot_general(a, b, (((1,), (1,)), ((), ())), preferred_element_type=F32)


def t_mm(a, b):
    return lax.dot_general(a, b, (((0,), (0,)), ((), ())), preferred_element_type=F32)


def iota(shape, dim):
    return lax.broadcasted_iota(jnp.int32, shape, dim)


def params(*semantics):
    if semantics:
        return pltpu.CompilerParams(dimension_semantics=semantics, vmem_limit_bytes=60 << 20)
    return pltpu.CompilerParams(vmem_limit_bytes=60 << 20)


def whole(shape):
    return pl.BlockSpec(shape, lambda *_: (0,) * len(shape))


SMEM_SPEC = pl.BlockSpec(memory_space=pltpu.SMEM)


def route_kernel(n, rows, width, me_ref, train_ref, ids_ref, gates_ref, up_ref, *outs):
    pick_ref, blocks = outs[0], outs[1:]
    ids = ids_ref[...]
    gates = gates_ref[...]
    me = me_ref[0]
    row_n = iota((n, rows), 0)
    hits = jnp.zeros((n, rows), F32)
    level = jnp.zeros((n, rows), F32)
    for k in range(n):
        j = me + k
        j = jnp.where(j >= n, j - n, j)
        same = ids == train_ref[j]
        hit = jnp.sum(same.astype(F32), axis=0, keepdims=True)
        gate = jnp.sum(jnp.where(same, gates, 0.0), axis=0, keepdims=True)
        hits = jnp.where(row_n == k, hit, hits)
        level = jnp.where(row_n == k, gate, level)
    before = (iota((rows, rows), 0) < iota((rows, rows), 1)).astype(BF16)
    rank = mm(hits.astype(BF16), before)
    place = jnp.where(hits > 0.5, rank, 1e4)
    sub = iota((PIECE, rows), 0)
    slot = jnp.where(sub >= CAP, sub - CAP, sub).astype(F32)
    firsts, seconds, scales = [], [], []
    for k in range(n):
        chosen = place[k : k + 1, :] == slot
        firsts.append(jnp.where(chosen & (sub < CAP), 1.0, 0.0))
        seconds.append(jnp.where(chosen & (sub >= CAP), 1.0, 0.0))
        scales.append(jnp.sum(jnp.where(chosen, level[k : k + 1, :], 0.0), axis=1, keepdims=True))
    first = jnp.concatenate(firsts, axis=0).astype(BF16)
    second = jnp.concatenate(seconds, axis=0).astype(BF16)
    scale = jnp.concatenate(scales, axis=0)
    pick_ref[0] = first
    pick_ref[1] = second
    half = width // FOLD
    chunk = min(512, half)
    for c in range(0, half, chunk):
        picked = mm(first, up_ref[:, c : c + chunk]) + mm(second, up_ref[:, half + c : half + c + chunk])
        picked = (picked * scale).astype(BF16)
        for k in range(n):
            blocks[k][:, c : c + chunk] = picked[k * PIECE : (k + 1) * PIECE]


def route(me, trainable, ids, gates, upstream):
    n = trainable.shape[0]
    rows, width = upstream.shape
    half = width // FOLD
    out_shape = [jax.ShapeDtypeStruct((2, n * PIECE, rows), BF16)] + [
        jax.ShapeDtypeStruct((PIECE, half), BF16) for _ in range(n)
    ]
    outs = pl.pallas_call(
        lambda *refs: route_kernel(n, rows, width, *refs),
        out_shape=out_shape,
        in_specs=[SMEM_SPEC, SMEM_SPEC] + [pl.BlockSpec(memory_space=pltpu.VMEM)] * 3,
        compiler_params=params(),
        cost_estimate=pl.CostEstimate(flops=4 * 10**9, bytes_accessed=2 * 10**6, transcendentals=0),
        name="route",
    )(me, trainable, ids, gates, upstream)
    return outs[0], list(outs[1:])


def unfold_kernel(n, slots, half, *refs):
    blocks, outs = refs[:n], refs[n:]
    r = iota((slots, n * PIECE), 0)
    s = iota((slots, n * PIECE), 1)
    start = r
    for k in range(1, n):
        start = start + jnp.where(r >= k * CAP, PIECE - CAP, 0)
    part = slots // 2
    chunk = min(512, half)
    for f in range(FOLD):
        select = (s == start + f * CAP).astype(BF16)
        for c in range(0, half, chunk):
            stacked = jnp.concatenate([b[:, c : c + chunk] for b in blocks], axis=0)
            got = mm(select, stacked).astype(BF16)
            at = f * half + c
            outs[0][:, at : at + chunk] = got[:part]
            outs[1][:, at : at + chunk] = got[part:]


def unfold(blocks):
    n = len(blocks)
    half = blocks[0].shape[1]
    slots = n * CAP
    return pl.pallas_call(
        lambda *refs: unfold_kernel(n, slots, half, *refs),
        out_shape=[jax.ShapeDtypeStruct((slots // 2, FOLD * half), BF16)] * 2,
        compiler_params=params(),
        cost_estimate=pl.CostEstimate(flops=2 * 10**9, bytes_accessed=10**6, transcendentals=0),
        name="unfold",
    )(*blocks)


def forward_kernel(n, rows, width, me_ref, span_ref, *refs):
    kv_refs = refs[:n]
    q_ref, pick_ref, gain_ref = refs[n : n + 3]
    ka_ref, va_ref, kt_ref, vt_ref, exp_ref, inv_ref, mixed_ref, factor_ref = refs[n + 3 : n + 11]
    blocks = refs[n + 11 : n + 11 + n]
    b_ref, all_ref = refs[n + 11 + n :]
    step = pl.program_id(0)
    total = n * rows
    half_rows = rows // 2
    per_step = STEP_HEADS * HEAD_SIZE
    groups = ka_ref.shape[0]

    @pl.when(step == 0)
    def _():
        me = me_ref[0]
        lane = iota((rows, rows), 1)
        sub = iota((rows, rows), 0)
        lane_half = (lane >= half_rows).astype(jnp.int32)
        sub_half = (sub >= half_rows).astype(jnp.int32)
        lane_in = lane - lane_half * half_rows
        sub_in = sub - sub_half * half_rows
        b_ref[...] = jnp.where((lane_half == sub_half) & (lane_in >= sub_in), MASK_FILLER, 0.0).astype(BF16)
        mine0 = span_ref[0, 2 * me]
        mine1 = span_ref[0, 2 * me + 1]
        lane_span = jnp.where(lane_half == 0, mine0, mine1)
        for b in range(n):
            source = source_of(me, b, n)
            sub_span = jnp.where(sub_half == 0, span_ref[0, 2 * source], span_ref[0, 2 * source + 1])
            hot = ((sub_span == lane_span) & (lane_in == sub_in - 1)) | (
                (sub_span > lane_span) & (lane_in == half_rows - 1)
            )
            hot = jnp.where(hot, 1.0, 0.0).astype(BF16)
            kv = kv_refs[b][...]
            at = slice(b * rows, (b + 1) * rows)
            for g in range(groups):
                key = kv[:, g * HEAD_SIZE : (g + 1) * HEAD_SIZE]
                value = kv[:, (groups + g) * HEAD_SIZE : (groups + g + 1) * HEAD_SIZE]
                ka_ref[g, at, :HEAD_SIZE] = key
                ka_ref[g, at, HEAD_SIZE:] = hot
                va_ref[g, at, :HEAD_SIZE] = value
                va_ref[g, at, HEAD_SIZE:] = jnp.full((rows, HEAD_SIZE), -1.0, BF16)
                kt_ref[g, :, at] = key.T
                vt_ref[g, :HEAD_SIZE, at] = value.T
                vt_ref[g, HEAD_SIZE:, at] = jnp.ones((16, rows), BF16)

    g = step // (HEADS_PER_GROUP // STEP_HEADS)
    b = b_ref[...]
    for p in range(STEP_HEADS // 2):
        at = p * 2 * HEAD_SIZE
        q0 = q_ref[:, at : at + HEAD_SIZE]
        q1 = q_ref[:, at + HEAD_SIZE : at + 2 * HEAD_SIZE]
        qb = jnp.concatenate(
            [jnp.concatenate([q0, b], axis=1), jnp.concatenate([q1, b], axis=1)], axis=0
        )
        scores = mm_t(ka_ref[g], qb)
        peak = jnp.max(scores, axis=0, keepdims=True)
        exps = jnp.exp2((scores - peak) * (SCALE * LOG2E)).astype(BF16)
        exp_ref[p] = exps
        out = mm(vt_ref[g], exps)
        inv = 1.0 / out[HEAD_SIZE : HEAD_SIZE + 1, :]
        normal = out[:HEAD_SIZE, :] * inv
        inv_full = jnp.broadcast_to(inv, (rows, 2 * rows))
        for i in range(2):
            cols = slice(at + i * HEAD_SIZE, at + (i + 1) * HEAD_SIZE)
            head = normal[:, i * rows : (i + 1) * rows].T.astype(BF16)
            mixed_ref[:, cols] = head
            all_ref[step, :, cols] = head
            inv_ref[:, cols] = inv_full[:, i * rows : (i + 1) * rows].T

    @pl.when(step == pl.num_programs(0) - 1)
    def _():
        steps = width // per_step
        square = jnp.zeros((rows, 1), F32)
        for i in range(steps):
            part = all_ref[i].astype(F32)
            square = square + jnp.sum(part * part, axis=1, keepdims=True)
        factor = lax.rsqrt(square / width + EPSILON)
        factor_ref[...] = jnp.broadcast_to(factor, (rows, 128))
        half = width // FOLD

        def normed(i):
            gain = gain_ref[:, i * per_step : (i + 1) * per_step]
            return (all_ref[i].astype(F32) * factor * gain).astype(BF16)

        for i in range(steps // FOLD):
            picked = mm(pick_ref[0], normed(i)) + mm(pick_ref[1], normed(steps // FOLD + i))
            picked = picked.astype(BF16)
            for k in range(n):
                blocks[k][:, i * per_step : (i + 1) * per_step] = picked[k * PIECE : (k + 1) * PIECE]


def source_of(me, b, n):
    core = me % 2
    chip = me // 2 - b // 2
    chip = jnp.where(chip < 0, chip + n // 2, chip)
    return 2 * chip + (core if b % 2 == 0 else 1 - core)


def forward(me, span, kv_blocks, query, pick, gain):
    n = len(kv_blocks)
    rows, width = query.shape
    groups = kv_blocks[0].shape[1] // (2 * HEAD_SIZE)
    total = n * rows
    per_step = STEP_HEADS * HEAD_SIZE
    steps = width // per_step
    half = width // FOLD
    pairs = width // (2 * HEAD_SIZE)
    out_shape = [
        jax.ShapeDtypeStruct((groups, total, 2 * HEAD_SIZE), BF16),
        jax.ShapeDtypeStruct((groups, total, 2 * HEAD_SIZE), BF16),
        jax.ShapeDtypeStruct((groups, HEAD_SIZE, total), BF16),
        jax.ShapeDtypeStruct((groups, HEAD_SIZE + 16, total), BF16),
        jax.ShapeDtypeStruct((pairs, total, 2 * rows), BF16),
        jax.ShapeDtypeStruct((rows, width), F32),
        jax.ShapeDtypeStruct((rows, width), BF16),
        jax.ShapeDtypeStruct((rows, 128), F32),
    ] + [jax.ShapeDtypeStruct((PIECE, half), BF16) for _ in range(n)]
    column = pl.BlockSpec((rows, per_step), lambda i: (0, i))
    out_specs = [whole(s.shape) for s in out_shape]
    out_specs[4] = pl.BlockSpec((STEP_HEADS // 2, total, 2 * rows), lambda i: (i, 0, 0))
    out_specs[5] = column
    out_specs[6] = column
    outs = pl.pallas_call(
        lambda *refs: forward_kernel(n, rows, width, *refs),
        out_shape=out_shape,
        grid=(steps,),
        in_specs=[SMEM_SPEC, SMEM_SPEC]
        + [whole(kv_blocks[0].shape)] * n
        + [column, whole(pick.shape), whole(gain.shape)],
        out_specs=out_specs,
        scratch_shapes=[pltpu.VMEM((rows, rows), BF16), pltpu.VMEM((steps, rows, per_step), BF16)],
        compiler_params=params("arbitrary"),
        cost_estimate=pl.CostEstimate(flops=10**10, bytes_accessed=2 * 10**7, transcendentals=4 * 10**6),
        name="forward",
    )(me, span, *kv_blocks, query, pick, gain)
    return outs[:8], list(outs[8:])


def gated(gate_in, up_in, back):
    sigma = 1.0 / (1.0 + jnp.exp(-gate_in))
    act = gate_in * sigma
    grad_gate = (back * up_in * sigma * (1.0 + gate_in * (1.0 - sigma))).astype(BF16)
    grad_up = (back * act).astype(BF16)
    product = (act * up_in).astype(BF16)
    return grad_gate, grad_up, product


def expert_kernel(n, slots, *refs):
    r0, r1, w0, w1, weights = refs[:5]
    blocks = refs[5 : 5 + n]
    rows_ref, grads_ref, acc_ref = refs[5 + n :]
    step = pl.program_id(0)
    width = acc_ref.shape[1]

    @pl.when(step == 0)
    def _():
        rows_ref[...] = jnp.concatenate([r0[...], r1[...]], axis=0)
        grads_ref[...] = jnp.concatenate([w0[...], w1[...]], axis=0)
        acc_ref[...] = jnp.zeros_like(acc_ref)

    routed = rows_ref[...]
    gate_in = mm_t(routed, weights[0])
    up_in = mm_t(routed, weights[1])
    back = mm_t(grads_ref[...], weights[2])
    grad_gate, grad_up, _ = gated(gate_in, up_in, back)
    acc_ref[...] += mm(grad_gate, weights[0]) + mm(grad_up, weights[1])

    @pl.when(step == pl.num_programs(0) - 1)
    def _():
        half = width // FOLD
        r = iota((n * PIECE, slots), 1)
        s = iota((n * PIECE, slots), 0)
        start = r
        for k in range(1, n):
            start = start + jnp.where(r >= k * CAP, PIECE - CAP, 0)
        first = (s == start).astype(BF16)
        second = (s == start + CAP).astype(BF16)
        chunk = min(512, half)
        for c in range(0, half, chunk):
            spread = mm(first, acc_ref[:, c : c + chunk].astype(BF16)) + mm(
                second, acc_ref[:, half + c : half + c + chunk].astype(BF16)
            )
            spread = spread.astype(BF16)
            for k in range(n):
                blocks[k][:, c : c + chunk] = spread[k * PIECE : (k + 1) * PIECE]


def expert(routed, weighted, weights, n):
    slots = n * CAP
    hidden, width = weights.shape[1:]
    tile = 128
    half = width // FOLD
    part = whole(routed[0].shape)
    return list(
        pl.pallas_call(
            lambda *refs: expert_kernel(n, slots, *refs),
            out_shape=[jax.ShapeDtypeStruct((PIECE, half), BF16)] * n,
            grid=(hidden // tile,),
            in_specs=[part] * 4 + [pl.BlockSpec((3, tile, width), lambda i: (0, i, 0))],
            out_specs=[whole((PIECE, half))] * n,
            scratch_shapes=[
                pltpu.VMEM((slots, width), BF16),
                pltpu.VMEM((slots, width), BF16),
                pltpu.VMEM((slots, width), F32),
            ],
            compiler_params=params("arbitrary"),
            cost_estimate=pl.CostEstimate(flops=8 * 10**9, bytes_accessed=2 * 10**7, transcendentals=0),
            name="expert",
        )(*routed, *weighted, weights)
    )


def grads_kernel(count, dp_ref, *refs):
    row_parts, grad_parts = refs[:count], refs[count : 2 * count]
    weights, out_ref, rows_ref, grads_ref, sems = refs[2 * count :]
    part = row_parts[0].shape[0]

    @pl.when(pl.program_id(0) == 0)
    def _():
        copies = []
        for i in range(count):
            at = pl.ds(i * part, part)
            copies.append(pltpu.make_async_copy(row_parts[i], rows_ref.at[at], sems.at[i]))
            copies.append(pltpu.make_async_copy(grad_parts[i], grads_ref.at[at], sems.at[count + i]))
        for copy in copies:
            copy.start()
        for copy in copies:
            copy.wait()

    rows = rows_ref[...]
    grads = grads_ref[...]
    gate_in = mm_t(rows, weights[0])
    up_in = mm_t(rows, weights[1])
    back = mm_t(grads, weights[2])
    grad_gate, grad_up, product = gated(gate_in, up_in, back)
    out_ref[0] = t_mm(grad_gate, rows).astype(BF16)
    out_ref[1] = t_mm(grad_up, rows).astype(BF16)
    out_ref[2] = t_mm(product, grads).astype(BF16)


def expert_gradients(dp_index, row_parts, grad_parts, weights, share):
    count = len(row_parts)
    width = weights.shape[2]
    tile = math.gcd(share, 64)
    steps = share // tile
    part = row_parts[0].shape
    return pl.pallas_call(
        lambda *refs: grads_kernel(count, *refs),
        out_shape=jax.ShapeDtypeStruct((3, share, width), BF16),
        grid_spec=pltpu.PrefetchScalarGridSpec(
            num_scalar_prefetch=1,
            grid=(steps,),
            in_specs=[pl.BlockSpec(memory_space=pl.ANY)] * (2 * count)
            + [pl.BlockSpec((3, tile, width), lambda i, d: (0, d[0] * steps + i, 0))],
            out_specs=pl.BlockSpec((3, tile, width), lambda i, d: (0, i, 0)),
            scratch_shapes=[pltpu.VMEM((count * part[0], width), BF16)] * 2
            + [pltpu.SemaphoreType.DMA((2 * count,))],
        ),
        compiler_params=params("arbitrary"),
        cost_estimate=pl.CostEstimate(flops=10**10, bytes_accessed=15 * 10**6, transcendentals=0),
        name="grads",
    )(dp_index, *row_parts, *grad_parts, weights)


def backward_kernel(n, rows, width, *refs):
    back_refs = refs[:n]
    pick_ref, up_ref, mixed_ref, gain_ref, factor_ref, q_ref, inv_ref, exp_ref, va_ref, kt_ref = refs[n : n + 10]
    dq_ref, near_ref, far_ref = refs[n + 10 : n + 13]
    gm_ref, ig_ref, dk_ref, dv_ref = refs[n + 13 :]
    step = pl.program_id(0)
    steps = pl.num_programs(0)
    per_step = STEP_HEADS * HEAD_SIZE
    per_group = HEADS_PER_GROUP // STEP_HEADS
    chunks = width // per_step
    g = step // per_group

    @pl.when(step == 0)
    def _():
        half_chunks = chunks // FOLD
        total = jnp.zeros((rows, 1), F32)
        for i in range(chunks):
            f, c = i // half_chunks, (i % half_chunks) * per_step
            stacked = jnp.concatenate([b[:, c : c + per_step] for b in back_refs], axis=0)
            grad = t_mm(pick_ref[f], stacked) * gain_ref[:, i * per_step : (i + 1) * per_step]
            ig_ref[i] = grad
            mixed = mixed_ref[:, i * per_step : (i + 1) * per_step].astype(F32)
            total = total + jnp.sum(grad * mixed, axis=1, keepdims=True)
        factor = factor_ref[:, :1]
        pull = factor * factor * factor * (total / width)
        for i in range(chunks):
            mixed = mixed_ref[:, i * per_step : (i + 1) * per_step].astype(F32)
            up = up_ref[:, i * per_step : (i + 1) * per_step].astype(F32)
            gm_ref[i] = (up + (factor * ig_ref[i] - mixed * pull)).astype(BF16)

    @pl.when(step % per_group == 0)
    def _():
        dk_ref[...] = jnp.zeros_like(dk_ref)
        dv_ref[...] = jnp.zeros_like(dv_ref)

    col = pl.multiple_of(step * per_step, per_step)
    grad_all = gm_ref[step].astype(F32) * inv_ref[...]
    grad_b = grad_all.astype(BF16)
    prod = (grad_b.astype(F32) * mixed_ref[:, pl.ds(col, per_step)].astype(F32)).astype(BF16)
    for p in range(STEP_HEADS // 2):
        at = p * 2 * HEAD_SIZE

        def stack(x):
            return jnp.concatenate([x[:, at : at + HEAD_SIZE], x[:, at + HEAD_SIZE : at + 2 * HEAD_SIZE]], axis=0)

        gs = stack(grad_b)
        gb = jnp.concatenate([gs, stack(prod)], axis=1)
        pushed = mm_t(va_ref[g], gb)
        exps = exp_ref[p]
        slopes = (exps.astype(F32) * pushed).astype(BF16)
        qs = jnp.concatenate([q_ref[:, at : at + HEAD_SIZE], q_ref[:, at + HEAD_SIZE : at + 2 * HEAD_SIZE]], axis=0)
        dk_ref[...] += mm(slopes, qs)
        dv_ref[...] += mm(exps, gs)
        dq = mm(kt_ref[g], slopes) * SCALE
        for i in range(2):
            cols = slice(at + i * HEAD_SIZE, at + (i + 1) * HEAD_SIZE)
            dq_ref[:, cols] = dq[:, i * rows : (i + 1) * rows].T.astype(BF16)

    groups = va_ref.shape[0]
    for gg in range(groups):

        @pl.when(step == (gg + 1) * per_group - 1)
        def _():
            for b in range(n):
                at = slice(b * rows, (b + 1) * rows)
                kcol = slice(gg * HEAD_SIZE, (gg + 1) * HEAD_SIZE)
                vcol = slice((groups + gg) * HEAD_SIZE, (groups + gg + 1) * HEAD_SIZE)
                if b % 2 == 0:
                    near_ref[b // 2, :, kcol] = dk_ref[at] * SCALE
                    near_ref[b // 2, :, vcol] = dv_ref[at]
                else:
                    far_ref[b // 2, :, kcol] = (dk_ref[at] * SCALE).astype(BF16)
                    far_ref[b // 2, :, vcol] = dv_ref[at].astype(BF16)


def backward(back, pick, upstream, gain, query, fwd):
    ka, va, kt, vt, exps, inv, mixed, factor = fwd
    n = len(back)
    rows, width = query.shape
    groups, total = va.shape[:2]
    per_step = STEP_HEADS * HEAD_SIZE
    steps = width // per_step
    column = pl.BlockSpec((rows, per_step), lambda i: (0, i))
    kv_width = 2 * groups * HEAD_SIZE
    return pl.pallas_call(
        lambda *refs: backward_kernel(n, rows, width, *refs),
        out_shape=[
            jax.ShapeDtypeStruct((rows, width), BF16),
            jax.ShapeDtypeStruct((n // 2, rows, kv_width), F32),
            jax.ShapeDtypeStruct((n // 2, rows, kv_width), BF16),
        ],
        grid=(steps,),
        in_specs=[whole(back[0].shape)] * n
        + [whole(pick.shape), whole(upstream.shape), whole(mixed.shape), whole(gain.shape), whole(factor.shape)]
        + [
            column,
            column,
            pl.BlockSpec((STEP_HEADS // 2, total, 2 * rows), lambda i: (i, 0, 0)),
            whole(va.shape),
            whole(kt.shape),
        ],
        out_specs=[column, whole((n // 2, rows, kv_width)), whole((n // 2, rows, kv_width))],
        scratch_shapes=[
            pltpu.VMEM((steps, rows, per_step), BF16),
            pltpu.VMEM((steps, rows, per_step), F32),
            pltpu.VMEM((total, HEAD_SIZE), F32),
            pltpu.VMEM((total, HEAD_SIZE), F32),
        ],
        compiler_params=params("arbitrary"),
        cost_estimate=pl.CostEstimate(flops=2 * 10**10, bytes_accessed=2 * 10**7, transcendentals=0),
        name="backward",
    )(*back, pick, upstream, mixed, gain, factor, query, inv, exps, va, kt)


def shift(x, axis, k):
    n = lax.axis_size(axis)
    return lax.ppermute(x, axis, [(i, (i + k) % n) for i in range(n)])


def flip(x, axis, bit):
    n = lax.axis_size(axis)
    return lax.ppermute(x, axis, [(i, i ^ bit) for i in range(n)])


def far_first(n):
    return sorted(range(1, n), key=lambda k: -min(k, n - k))


def exchange(blocks, sign):
    n = len(blocks)
    got = [blocks[0]] + [None] * (n - 1)
    for k in far_first(n):
        got[k] = shift(blocks[k], "ctx", sign * k)
    return got


def gather_docs(parts):
    n = lax.axis_size("dp")
    bits = [1 << b for b in range(n.bit_length() - 1)]
    first, second = [parts[0]], [parts[1]]
    for a, b in zip(bits, bits[::-1]):
        moved_first = [flip(x, "dp", a) for x in first]
        moved_second = [flip(x, "dp", b) for x in second]
        first += moved_first
        second += moved_second
    return first + second


def per_device(
    query,
    key,
    value,
    span_order,
    expert_ids,
    expert_gates,
    trainable,
    norm_gain,
    upstream,
    expert_weights,
):
    n = lax.axis_size("ctx")
    chips = n // 2
    me = lax.axis_index("ctx").astype(jnp.int32).reshape(1)
    dp_index = lax.axis_index("dp").astype(jnp.int32).reshape(1)
    weights = expert_weights[0].transpose(1, 0, 2)
    gain = norm_gain[None, :]
    grad_out = upstream[0]

    kv = jnp.concatenate([key[0], value[0]], axis=1)
    arrived = [kv] + [shift(kv, "ctx", 2 * m) for m in range(1, chips)]
    kv_blocks = []
    for block in arrived:
        kv_blocks += [block, flip(block, "ctx", 1)]

    pick, grad_blocks = route(me, trainable, expert_ids[0].T, expert_gates[0].T, grad_out)
    weighted = unfold(exchange(grad_blocks, 1))
    all_weighted = gather_docs(weighted)

    fwd, row_blocks = forward(me, span_order, kv_blocks, query[0], pick, gain)
    routed = unfold(exchange(row_blocks, 1))
    all_routed = gather_docs(routed)
    returned = expert(routed, weighted, weights, n)
    back = exchange(returned, -1)
    share = weights.shape[1] // lax.axis_size("dp")
    expert_grads = expert_gradients(dp_index, all_routed, all_weighted, weights, share)
    d_query, near, far = backward(back, pick, grad_out, gain, query[0], fwd)

    met = near + flip(far, "ctx", 1).astype(F32)
    total = met[0]
    sent = met.astype(BF16)
    for m in range(1, chips):
        total = total + shift(sent[m], "ctx", -2 * m).astype(F32)
    split = key.shape[2]
    return (
        d_query[None],
        total[:, :split].astype(BF16)[None],
        total[:, split:].astype(BF16)[None],
        expert_grads.transpose(1, 0, 2)[None],
    )


def solution(mesh):
    in_specs = (
        P("dp", "ctx", None),
        P("dp", "ctx", None),
        P("dp", "ctx", None),
        P("dp", None),
        P("dp", "ctx", None),
        P("dp", "ctx", None),
        P(),
        P(),
        P("dp", "ctx", None),
        P("ctx", None, None, None),
    )
    out_specs = (
        P("dp", "ctx", None),
        P("dp", "ctx", None),
        P("dp", "ctx", None),
        P("ctx", "dp", None, None),
    )
    return jax.shard_map(
        per_device, mesh=mesh, in_specs=in_specs, out_specs=out_specs, check_vma=False
    )
```

```python
import jax
import jax.numpy as jnp
from jax import lax
from jax.experimental import pallas as pl
from jax.experimental.pallas import tpu as pltpu
from jax.sharding import PartitionSpec as P


HEADS_PER_GROUP = 16
HEAD_SIZE = 128
CAP = 12
EPSILON = 1e-06
MASK_FILLER = -1e30
SCALE = HEAD_SIZE ** (-0.5)
LOG2E = 1.4426950408889634
FOLD = 2
PIECE = FOLD * CAP
STEP_HEADS = 4
F32 = jnp.float32
BF16 = jnp.bfloat16


def mm(a, b):
    return lax.dot_general(a, b, (((1,), (0,)), ((), ())), preferred_element_type=F32)


def mm_t(a, b):
    return lax.dot_general(a, b, (((1,), (1,)), ((), ())), preferred_element_type=F32)


def t_mm(a, b):
    return lax.dot_general(a, b, (((0,), (0,)), ((), ())), preferred_element_type=F32)


def iota(shape, dim):
    return lax.broadcasted_iota(jnp.int32, shape, dim)


def params(*semantics):
    if semantics:
        return pltpu.CompilerParams(dimension_semantics=semantics, vmem_limit_bytes=60 << 20)
    return pltpu.CompilerParams(vmem_limit_bytes=60 << 20)


def whole(shape):
    return pl.BlockSpec(shape, lambda *_: (0,) * len(shape))


SMEM_SPEC = pl.BlockSpec(memory_space=pltpu.SMEM)


def route_kernel(n, rows, width, me_ref, train_ref, ids_ref, gates_ref, up_ref, *outs):
    pick_ref, blocks = outs[0], outs[1:]
    ids = ids_ref[...]
    gates = gates_ref[...]
    me = me_ref[0]
    row_n = iota((n, rows), 0)
    hits = jnp.zeros((n, rows), F32)
    level = jnp.zeros((n, rows), F32)
    for k in range(n):
        j = me + k
        j = jnp.where(j >= n, j - n, j)
        same = ids == train_ref[j]
        hit = jnp.sum(same.astype(F32), axis=0, keepdims=True)
        gate = jnp.sum(jnp.where(same, gates, 0.0), axis=0, keepdims=True)
        hits = jnp.where(row_n == k, hit, hits)
        level = jnp.where(row_n == k, gate, level)
    before = (iota((rows, rows), 0) < iota((rows, rows), 1)).astype(BF16)
    rank = mm(hits.astype(BF16), before)
    place = jnp.where(hits > 0.5, rank, 1e4)
    sub = iota((PIECE, rows), 0)
    slot = jnp.where(sub >= CAP, sub - CAP, sub).astype(F32)
    firsts, seconds, scales = [], [], []
    for k in range(n):
        chosen = place[k : k + 1, :] == slot
        firsts.append(jnp.where(chosen & (sub < CAP), 1.0, 0.0))
        seconds.append(jnp.where(chosen & (sub >= CAP), 1.0, 0.0))
        scales.append(jnp.sum(jnp.where(chosen, level[k : k + 1, :], 0.0), axis=1, keepdims=True))
    first = jnp.concatenate(firsts, axis=0).astype(BF16)
    second = jnp.concatenate(seconds, axis=0).astype(BF16)
    scale = jnp.concatenate(scales, axis=0)
    pick_ref[0] = first
    pick_ref[1] = second
    half = width // FOLD
    chunk = min(512, half)
    for c in range(0, half, chunk):
        picked = mm(first, up_ref[:, c : c + chunk]) + mm(second, up_ref[:, half + c : half + c + chunk])
        picked = (picked * scale).astype(BF16)
        for k in range(n):
            blocks[k][:, c : c + chunk] = picked[k * PIECE : (k + 1) * PIECE]


def route(me, trainable, ids, gates, upstream):
    n = trainable.shape[0]
    rows, width = upstream.shape
    half = width // FOLD
    out_shape = [jax.ShapeDtypeStruct((2, n * PIECE, rows), BF16)] + [
        jax.ShapeDtypeStruct((PIECE, half), BF16) for _ in range(n)
    ]
    outs = pl.pallas_call(
        lambda *refs: route_kernel(n, rows, width, *refs),
        out_shape=out_shape,
        in_specs=[SMEM_SPEC, SMEM_SPEC] + [pl.BlockSpec(memory_space=pltpu.VMEM)] * 3,
        compiler_params=params(),
        cost_estimate=pl.CostEstimate(flops=4 * 10**9, bytes_accessed=2 * 10**6, transcendentals=0),
        name="route",
    )(me, trainable, ids, gates, upstream)
    return outs[0], list(outs[1:])


def unfold_kernel(n, slots, half, *refs):
    blocks, out_ref = refs[:n], refs[n]
    r = iota((slots, n * PIECE), 0)
    s = iota((slots, n * PIECE), 1)
    start = r
    for k in range(1, n):
        start = start + jnp.where(r >= k * CAP, PIECE - CAP, 0)
    chunk = min(512, half)
    for f in range(FOLD):
        select = (s == start + f * CAP).astype(BF16)
        for c in range(0, half, chunk):
            stacked = jnp.concatenate([b[:, c : c + chunk] for b in blocks], axis=0)
            at = f * half + c
            out_ref[:, at : at + chunk] = mm(select, stacked).astype(BF16)


def unfold(blocks):
    n = len(blocks)
    half = blocks[0].shape[1]
    slots = n * CAP
    return pl.pallas_call(
        lambda *refs: unfold_kernel(n, slots, half, *refs),
        out_shape=jax.ShapeDtypeStruct((slots, FOLD * half), BF16),
        compiler_params=params(),
        cost_estimate=pl.CostEstimate(flops=2 * 10**9, bytes_accessed=10**6, transcendentals=0),
        name="unfold",
    )(*blocks)


def forward_kernel(n, rows, width, me_ref, span_ref, *refs):
    kv_refs = refs[:n]
    q_ref, pick_ref, gain_ref = refs[n : n + 3]
    ka_ref, va_ref, kt_ref, vt_ref, exp_ref, inv_ref, mixed_ref, factor_ref = refs[n + 3 : n + 11]
    blocks = refs[n + 11 : n + 11 + n]
    b_ref, all_ref = refs[n + 11 + n :]
    step = pl.program_id(0)
    half_rows = rows // 2
    per_step = STEP_HEADS * HEAD_SIZE
    groups = ka_ref.shape[0]

    @pl.when(step == 0)
    def _():
        me = me_ref[0]
        lane = iota((rows, rows), 1)
        sub = iota((rows, rows), 0)
        lane_half = (lane >= half_rows).astype(jnp.int32)
        sub_half = (sub >= half_rows).astype(jnp.int32)
        lane_in = lane - lane_half * half_rows
        sub_in = sub - sub_half * half_rows
        b_ref[...] = jnp.where((lane_half == sub_half) & (lane_in >= sub_in), MASK_FILLER, 0.0).astype(BF16)
        mine0 = span_ref[0, 2 * me]
        mine1 = span_ref[0, 2 * me + 1]
        lane_span = jnp.where(lane_half == 0, mine0, mine1)
        for b in range(n):
            source = source_of(me, b, n)
            sub_span = jnp.where(sub_half == 0, span_ref[0, 2 * source], span_ref[0, 2 * source + 1])
            hot = ((sub_span == lane_span) & (lane_in == sub_in - 1)) | (
                (sub_span > lane_span) & (lane_in == half_rows - 1)
            )
            hot = jnp.where(hot, 1.0, 0.0).astype(BF16)
            kv = kv_refs[b][...]
            at = slice(b * rows, (b + 1) * rows)
            for g in range(groups):
                key = kv[:, g * HEAD_SIZE : (g + 1) * HEAD_SIZE]
                value = kv[:, (groups + g) * HEAD_SIZE : (groups + g + 1) * HEAD_SIZE]
                ka_ref[g, at, :HEAD_SIZE] = key
                ka_ref[g, at, HEAD_SIZE:] = hot
                va_ref[g, at, :HEAD_SIZE] = value
                va_ref[g, at, HEAD_SIZE:] = jnp.full((rows, HEAD_SIZE), -1.0, BF16)
                kt_ref[g, :, at] = key.T
                vt_ref[g, :HEAD_SIZE, at] = value.T
                vt_ref[g, HEAD_SIZE:, at] = jnp.ones((16, rows), BF16)

    g = step // (HEADS_PER_GROUP // STEP_HEADS)
    b = b_ref[...]
    for p in range(STEP_HEADS // 2):
        at = p * 2 * HEAD_SIZE
        q0 = q_ref[:, at : at + HEAD_SIZE]
        q1 = q_ref[:, at + HEAD_SIZE : at + 2 * HEAD_SIZE]
        qb = jnp.concatenate(
            [jnp.concatenate([q0, b], axis=1), jnp.concatenate([q1, b], axis=1)], axis=0
        )
        scores = mm_t(ka_ref[g], qb)
        peak = jnp.max(scores, axis=0, keepdims=True)
        exps = jnp.exp2((scores - peak) * (SCALE * LOG2E)).astype(BF16)
        exp_ref[p] = exps
        out = mm(vt_ref[g], exps)
        inv = 1.0 / out[HEAD_SIZE : HEAD_SIZE + 1, :]
        normal = out[:HEAD_SIZE, :] * inv
        inv_full = jnp.broadcast_to(inv, (rows, 2 * rows))
        for i in range(2):
            cols = slice(at + i * HEAD_SIZE, at + (i + 1) * HEAD_SIZE)
            head = normal[:, i * rows : (i + 1) * rows].T.astype(BF16)
            mixed_ref[:, cols] = head
            all_ref[step, :, cols] = head
            inv_ref[:, cols] = inv_full[:, i * rows : (i + 1) * rows].T

    @pl.when(step == pl.num_programs(0) - 1)
    def _():
        steps = width // per_step
        square = jnp.zeros((rows, 1), F32)
        for i in range(steps):
            part = all_ref[i].astype(F32)
            square = square + jnp.sum(part * part, axis=1, keepdims=True)
        factor = lax.rsqrt(square / width + EPSILON)
        factor_ref[...] = jnp.broadcast_to(factor, (rows, 128))

        def normed(i):
            gain = gain_ref[:, i * per_step : (i + 1) * per_step]
            return (all_ref[i].astype(F32) * factor * gain).astype(BF16)

        for i in range(steps // FOLD):
            picked = mm(pick_ref[0], normed(i)) + mm(pick_ref[1], normed(steps // FOLD + i))
            picked = picked.astype(BF16)
            for k in range(n):
                blocks[k][:, i * per_step : (i + 1) * per_step] = picked[k * PIECE : (k + 1) * PIECE]


def source_of(me, b, n):
    core = me % 2
    chip = me // 2 - b // 2
    chip = jnp.where(chip < 0, chip + n // 2, chip)
    return 2 * chip + (core if b % 2 == 0 else 1 - core)


def forward(me, span, kv_blocks, query, pick, gain):
    n = len(kv_blocks)
    rows, width = query.shape
    groups = kv_blocks[0].shape[1] // (2 * HEAD_SIZE)
    total = n * rows
    per_step = STEP_HEADS * HEAD_SIZE
    steps = width // per_step
    half = width // FOLD
    pairs = width // (2 * HEAD_SIZE)
    out_shape = [
        jax.ShapeDtypeStruct((groups, total, 2 * HEAD_SIZE), BF16),
        jax.ShapeDtypeStruct((groups, total, 2 * HEAD_SIZE), BF16),
        jax.ShapeDtypeStruct((groups, HEAD_SIZE, total), BF16),
        jax.ShapeDtypeStruct((groups, HEAD_SIZE + 16, total), BF16),
        jax.ShapeDtypeStruct((pairs, total, 2 * rows), BF16),
        jax.ShapeDtypeStruct((rows, width), F32),
        jax.ShapeDtypeStruct((rows, width), BF16),
        jax.ShapeDtypeStruct((rows, 128), F32),
    ] + [jax.ShapeDtypeStruct((PIECE, half), BF16) for _ in range(n)]
    column = pl.BlockSpec((rows, per_step), lambda i: (0, i))
    out_specs = [whole(s.shape) for s in out_shape]
    out_specs[4] = pl.BlockSpec((STEP_HEADS // 2, total, 2 * rows), lambda i: (i, 0, 0))
    out_specs[5] = column
    out_specs[6] = column
    outs = pl.pallas_call(
        lambda *refs: forward_kernel(n, rows, width, *refs),
        out_shape=out_shape,
        grid=(steps,),
        in_specs=[SMEM_SPEC, SMEM_SPEC]
        + [whole(kv_blocks[0].shape)] * n
        + [column, whole(pick.shape), whole(gain.shape)],
        out_specs=out_specs,
        scratch_shapes=[pltpu.VMEM((rows, rows), BF16), pltpu.VMEM((steps, rows, per_step), BF16)],
        compiler_params=params("arbitrary"),
        cost_estimate=pl.CostEstimate(flops=10**10, bytes_accessed=2 * 10**7, transcendentals=4 * 10**6),
        name="forward",
    )(me, span, *kv_blocks, query, pick, gain)
    return outs[:8], list(outs[8:])


def gated(gate_in, up_in, back):
    sigma = 1.0 / (1.0 + jnp.exp(-gate_in))
    act = gate_in * sigma
    grad_gate = (back * up_in * sigma * (1.0 + gate_in * (1.0 - sigma))).astype(BF16)
    grad_up = (back * act).astype(BF16)
    product = (act * up_in).astype(BF16)
    return grad_gate, grad_up, product


def early_kernel(grads_ref, weights, back_ref):
    back_ref[...] = mm_t(grads_ref[...], weights[0])


def early(weighted, weights):
    hidden, width = weights.shape[1:]
    slots = weighted.shape[0]
    tile = 256
    return pl.pallas_call(
        early_kernel,
        out_shape=jax.ShapeDtypeStruct((slots, hidden), F32),
        grid=(hidden // tile,),
        in_specs=[whole(weighted.shape), pl.BlockSpec((1, tile, width), lambda i: (2, i, 0))],
        out_specs=pl.BlockSpec((slots, tile), lambda i: (0, i)),
        compiler_params=params("arbitrary"),
        cost_estimate=pl.CostEstimate(flops=2 * 10**9, bytes_accessed=7 * 10**6, transcendentals=0),
        name="early",
    )(weighted, weights)


def expert_kernel(n, slots, routed_ref, back_ref, weights, *refs):
    blocks, acc_ref = refs[:n], refs[n]
    step = pl.program_id(0)
    width = acc_ref.shape[1]
    routed = routed_ref[...]
    gate_in = mm_t(routed, weights[0])
    up_in = mm_t(routed, weights[1])
    grad_gate, grad_up, _ = gated(gate_in, up_in, back_ref[...])
    got = mm(grad_gate, weights[0]) + mm(grad_up, weights[1])

    @pl.when(step == 0)
    def _():
        acc_ref[...] = got

    @pl.when(step > 0)
    def _():
        acc_ref[...] += got

    @pl.when(step == pl.num_programs(0) - 1)
    def _():
        half = width // FOLD
        r = iota((n * PIECE, slots), 1)
        s = iota((n * PIECE, slots), 0)
        start = r
        for k in range(1, n):
            start = start + jnp.where(r >= k * CAP, PIECE - CAP, 0)
        first = (s == start).astype(BF16)
        second = (s == start + CAP).astype(BF16)
        chunk = min(512, half)
        for c in range(0, half, chunk):
            spread = mm(first, acc_ref[:, c : c + chunk].astype(BF16)) + mm(
                second, acc_ref[:, half + c : half + c + chunk].astype(BF16)
            )
            spread = spread.astype(BF16)
            for k in range(n):
                blocks[k][:, c : c + chunk] = spread[k * PIECE : (k + 1) * PIECE]


def expert(routed, back, weights, n):
    slots = n * CAP
    hidden, width = weights.shape[1:]
    tile = 256
    half = width // FOLD
    return list(
        pl.pallas_call(
            lambda *refs: expert_kernel(n, slots, *refs),
            out_shape=[jax.ShapeDtypeStruct((PIECE, half), BF16)] * n,
            grid=(hidden // tile,),
            in_specs=[
                whole(routed.shape),
                pl.BlockSpec((slots, tile), lambda i: (0, i)),
                pl.BlockSpec((2, tile, width), lambda i: (0, i, 0)),
            ],
            out_specs=[whole((PIECE, half))] * n,
            scratch_shapes=[pltpu.VMEM((slots, width), F32)],
            compiler_params=params("arbitrary"),
            cost_estimate=pl.CostEstimate(flops=8 * 10**9, bytes_accessed=2 * 10**7, transcendentals=0),
            name="expert",
        )(routed, back, weights)
    )


def grads_kernel(count, dp_ref, *refs):
    row_parts, grad_parts = refs[:count], refs[count : 2 * count]
    weights, out_ref, rows_ref, grads_ref, sems = refs[2 * count :]
    part = row_parts[0].shape[0]

    @pl.when(pl.program_id(0) == 0)
    def _():
        copies = []
        for i in range(count):
            at = pl.ds(i * part, part)
            copies.append(pltpu.make_async_copy(row_parts[i], rows_ref.at[at], sems.at[i]))
            copies.append(pltpu.make_async_copy(grad_parts[i], grads_ref.at[at], sems.at[count + i]))
        for copy in copies:
            copy.start()
        for copy in copies:
            copy.wait()

    rows = rows_ref[...]
    grads = grads_ref[...]
    gate_in = mm_t(rows, weights[0])
    up_in = mm_t(rows, weights[1])
    back = mm_t(grads, weights[2])
    grad_gate, grad_up, product = gated(gate_in, up_in, back)
    out_ref[0] = t_mm(grad_gate, rows).astype(BF16)
    out_ref[1] = t_mm(grad_up, rows).astype(BF16)
    out_ref[2] = t_mm(product, grads).astype(BF16)


def expert_gradients(dp_index, row_parts, grad_parts, weights, share):
    count = len(row_parts)
    width = weights.shape[2]
    tile = share
    steps = share // tile
    part = row_parts[0].shape
    return pl.pallas_call(
        lambda *refs: grads_kernel(count, *refs),
        out_shape=jax.ShapeDtypeStruct((3, share, width), BF16),
        grid_spec=pltpu.PrefetchScalarGridSpec(
            num_scalar_prefetch=1,
            grid=(steps,),
            in_specs=[pl.BlockSpec(memory_space=pl.ANY)] * (2 * count)
            + [pl.BlockSpec((3, tile, width), lambda i, d: (0, d[0] * steps + i, 0))],
            out_specs=pl.BlockSpec((3, tile, width), lambda i, d: (0, i, 0)),
            scratch_shapes=[pltpu.VMEM((count * part[0], width), BF16)] * 2
            + [pltpu.SemaphoreType.DMA((2 * count,))],
        ),
        compiler_params=params("arbitrary"),
        cost_estimate=pl.CostEstimate(flops=10**10, bytes_accessed=15 * 10**6, transcendentals=0),
        name="grads",
    )(dp_index, *row_parts, *grad_parts, weights)


def backward_kernel(n, rows, width, *refs):
    back_refs = refs[:n]
    pick_ref, up_ref, mixed_ref, gain_ref, factor_ref, q_ref, inv_ref, exp_ref, va_ref, kt_ref = refs[n : n + 10]
    dq_ref, near_ref, far_ref = refs[n + 10 : n + 13]
    gm_ref, ig_ref, dk_ref, dv_ref = refs[n + 13 :]
    step = pl.program_id(0)
    per_step = STEP_HEADS * HEAD_SIZE
    per_group = HEADS_PER_GROUP // STEP_HEADS
    chunks = width // per_step
    g = step // per_group

    @pl.when(step == 0)
    def _():
        half_chunks = chunks // FOLD
        total = jnp.zeros((rows, 1), F32)
        for i in range(chunks):
            f, c = i // half_chunks, (i % half_chunks) * per_step
            stacked = jnp.concatenate([b[:, c : c + per_step] for b in back_refs], axis=0)
            grad = t_mm(pick_ref[f], stacked) * gain_ref[:, i * per_step : (i + 1) * per_step]
            ig_ref[i] = grad
            mixed = mixed_ref[:, i * per_step : (i + 1) * per_step].astype(F32)
            total = total + jnp.sum(grad * mixed, axis=1, keepdims=True)
        factor = factor_ref[:, :1]
        pull = factor * factor * factor * (total / width)
        for i in range(chunks):
            mixed = mixed_ref[:, i * per_step : (i + 1) * per_step].astype(F32)
            up = up_ref[:, i * per_step : (i + 1) * per_step].astype(F32)
            gm_ref[i] = (up + (factor * ig_ref[i] - mixed * pull)).astype(BF16)

    @pl.when(step % per_group == 0)
    def _():
        dk_ref[...] = jnp.zeros_like(dk_ref)
        dv_ref[...] = jnp.zeros_like(dv_ref)

    col = pl.multiple_of(step * per_step, per_step)
    grad_all = gm_ref[step].astype(F32) * inv_ref[...]
    grad_b = grad_all.astype(BF16)
    prod = (grad_b.astype(F32) * mixed_ref[:, pl.ds(col, per_step)].astype(F32)).astype(BF16)
    for p in range(STEP_HEADS // 2):
        at = p * 2 * HEAD_SIZE

        def stack(x):
            return jnp.concatenate([x[:, at : at + HEAD_SIZE], x[:, at + HEAD_SIZE : at + 2 * HEAD_SIZE]], axis=0)

        gs = stack(grad_b)
        gb = jnp.concatenate([gs, stack(prod)], axis=1)
        pushed = mm_t(va_ref[g], gb)
        exps = exp_ref[p]
        slopes = (exps.astype(F32) * pushed).astype(BF16)
        qs = jnp.concatenate([q_ref[:, at : at + HEAD_SIZE], q_ref[:, at + HEAD_SIZE : at + 2 * HEAD_SIZE]], axis=0)
        dk_ref[...] += mm(slopes, qs)
        dv_ref[...] += mm(exps, gs)
        dq = mm(kt_ref[g], slopes) * SCALE
        for i in range(2):
            cols = slice(at + i * HEAD_SIZE, at + (i + 1) * HEAD_SIZE)
            dq_ref[:, cols] = dq[:, i * rows : (i + 1) * rows].T.astype(BF16)

    groups = va_ref.shape[0]
    for gg in range(groups):

        @pl.when(step == (gg + 1) * per_group - 1)
        def _():
            for b in range(n):
                at = slice(b * rows, (b + 1) * rows)
                kcol = slice(gg * HEAD_SIZE, (gg + 1) * HEAD_SIZE)
                vcol = slice((groups + gg) * HEAD_SIZE, (groups + gg + 1) * HEAD_SIZE)
                if b % 2 == 0:
                    near_ref[b // 2, :, kcol] = dk_ref[at] * SCALE
                    near_ref[b // 2, :, vcol] = dv_ref[at]
                else:
                    far_ref[b // 2, :, kcol] = (dk_ref[at] * SCALE).astype(BF16)
                    far_ref[b // 2, :, vcol] = dv_ref[at].astype(BF16)


def backward(back, pick, upstream, gain, query, fwd):
    _, va, kt, _, exps, inv, mixed, factor = fwd
    n = len(back)
    rows, width = query.shape
    groups, total = va.shape[:2]
    per_step = STEP_HEADS * HEAD_SIZE
    steps = width // per_step
    column = pl.BlockSpec((rows, per_step), lambda i: (0, i))
    kv_width = 2 * groups * HEAD_SIZE
    return pl.pallas_call(
        lambda *refs: backward_kernel(n, rows, width, *refs),
        out_shape=[
            jax.ShapeDtypeStruct((rows, width), BF16),
            jax.ShapeDtypeStruct((n // 2, rows, kv_width), F32),
            jax.ShapeDtypeStruct((n // 2, rows, kv_width), BF16),
        ],
        grid=(steps,),
        in_specs=[whole(back[0].shape)] * n
        + [whole(pick.shape), whole(upstream.shape), whole(mixed.shape), whole(gain.shape), whole(factor.shape)]
        + [
            column,
            column,
            pl.BlockSpec((STEP_HEADS // 2, total, 2 * rows), lambda i: (i, 0, 0)),
            whole(va.shape),
            whole(kt.shape),
        ],
        out_specs=[column, whole((n // 2, rows, kv_width)), whole((n // 2, rows, kv_width))],
        scratch_shapes=[
            pltpu.VMEM((steps, rows, per_step), BF16),
            pltpu.VMEM((steps, rows, per_step), F32),
            pltpu.VMEM((total, HEAD_SIZE), F32),
            pltpu.VMEM((total, HEAD_SIZE), F32),
        ],
        compiler_params=params("arbitrary"),
        cost_estimate=pl.CostEstimate(flops=2 * 10**10, bytes_accessed=2 * 10**7, transcendentals=0),
        name="backward",
    )(*back, pick, upstream, mixed, gain, factor, query, inv, exps, va, kt)


def shift(x, axis, k):
    n = lax.axis_size(axis)
    return lax.ppermute(x, axis, [(i, (i + k) % n) for i in range(n)])


def flip(x, axis, bit):
    n = lax.axis_size(axis)
    return lax.ppermute(x, axis, [(i, i ^ bit) for i in range(n)])


def far_first(n):
    return sorted(range(1, n), key=lambda k: -min(k, n - k))


def exchange(blocks, sign):
    n = len(blocks)
    got = [blocks[0]] + [None] * (n - 1)
    for k in far_first(n):
        got[k] = shift(blocks[k], "ctx", sign * k)
    return got


def gather_docs(rows):
    n = lax.axis_size("dp")
    return [rows] + [flip(rows, "dp", k) for k in range(n - 1, 0, -1)]


def per_device(
    query,
    key,
    value,
    span_order,
    expert_ids,
    expert_gates,
    trainable,
    norm_gain,
    upstream,
    expert_weights,
):
    n = lax.axis_size("ctx")
    chips = n // 2
    me = lax.axis_index("ctx").astype(jnp.int32).reshape(1)
    dp_index = lax.axis_index("dp").astype(jnp.int32).reshape(1)
    weights = expert_weights[0].transpose(1, 0, 2)
    gain = norm_gain[None, :]
    grad_out = upstream[0]

    kv = jnp.concatenate([key[0], value[0]], axis=1)
    arrived = [kv] + [shift(kv, "ctx", 2 * m) for m in range(1, chips)]
    kv_blocks = []
    for block in arrived:
        kv_blocks += [block, flip(block, "ctx", 1)]

    pick, grad_blocks = route(me, trainable, expert_ids[0].T, expert_gates[0].T, grad_out)
    grad_blocks = exchange(grad_blocks, 1)
    weighted = unfold(grad_blocks)
    all_weighted = gather_docs(weighted)
    back_rows = early(weighted, weights)

    fwd, row_blocks = forward(me, span_order, kv_blocks, query[0], pick, gain)
    row_blocks = exchange(row_blocks, 1)
    routed = unfold(row_blocks)
    all_routed = gather_docs(routed)
    returned = expert(routed, back_rows, weights, n)
    back = exchange(returned, -1)
    share = weights.shape[1] // lax.axis_size("dp")
    expert_grads = expert_gradients(dp_index, all_routed, all_weighted, weights, share)
    d_query, near, far = backward(back, pick, grad_out, gain, query[0], fwd)

    far = flip(far, "ctx", 1)
    met = near + far.astype(F32)
    total = met[0]
    sent = met.astype(BF16)
    landed = [shift(sent[m], "ctx", -2 * m) for m in range(1, chips)]
    for block in landed:
        total = total + block.astype(F32)
    split = key.shape[2]
    return (
        d_query[None],
        total[:, :split].astype(BF16)[None],
        total[:, split:].astype(BF16)[None],
        expert_grads.transpose(1, 0, 2)[None],
    )


def solution(mesh):
    in_specs = (
        P("dp", "ctx", None),
        P("dp", "ctx", None),
        P("dp", "ctx", None),
        P("dp", None),
        P("dp", "ctx", None),
        P("dp", "ctx", None),
        P(),
        P(),
        P("dp", "ctx", None),
        P("ctx", None, None, None),
    )
    out_specs = (
        P("dp", "ctx", None),
        P("dp", "ctx", None),
        P("dp", "ctx", None),
        P("ctx", "dp", None, None),
    )

    return jax.shard_map(per_device, mesh=mesh, in_specs=in_specs, out_specs=out_specs, check_vma=False)
```

```python
import jax
import jax.numpy as jnp
from jax import lax
from jax.experimental import pallas as pl
from jax.experimental.pallas import tpu as pltpu
from jax.sharding import PartitionSpec as P


HEADS_PER_GROUP = 16
HEAD_SIZE = 128
CAP = 12
EPSILON = 1e-06
MASK_FILLER = -1e30
SCALE = HEAD_SIZE ** (-0.5)
LOG2E = 1.4426950408889634
FOLD = 2
PIECE = FOLD * CAP
STEP_HEADS = 8
F32 = jnp.float32
BF16 = jnp.bfloat16


def mm(a, b):
    return lax.dot_general(a, b, (((1,), (0,)), ((), ())), preferred_element_type=F32)


def mm_t(a, b):
    return lax.dot_general(a, b, (((1,), (1,)), ((), ())), preferred_element_type=F32)


def t_mm(a, b):
    return lax.dot_general(a, b, (((0,), (0,)), ((), ())), preferred_element_type=F32)


def iota(shape, dim):
    return lax.broadcasted_iota(jnp.int32, shape, dim)


def params(*semantics):
    if semantics:
        return pltpu.CompilerParams(dimension_semantics=semantics, vmem_limit_bytes=60 << 20)
    return pltpu.CompilerParams(vmem_limit_bytes=60 << 20)


def whole(shape):
    return pl.BlockSpec(shape, lambda *_: (0,) * len(shape))


SMEM_SPEC = pl.BlockSpec(memory_space=pltpu.SMEM)


def peer_of(me, b, n, sign):
    core = me % 2
    chip = (me // 2 + sign * (b // 2) + n // 2) % (n // 2)
    return 2 * chip + (core if b % 2 == 0 else 1 - core)


def route_kernel(n, rows, width, me_ref, train_ref, ids_ref, gates_ref, up_ref, *outs):
    pick_ref, blocks = outs[0], outs[1:]
    ids = ids_ref[...]
    gates = gates_ref[...]
    me = me_ref[0]
    row_n = iota((n, rows), 0)
    hits = jnp.zeros((n, rows), F32)
    level = jnp.zeros((n, rows), F32)
    for k in range(n):
        same = ids == train_ref[peer_of(me, k, n, 1)]
        hit = jnp.sum(same.astype(F32), axis=0, keepdims=True)
        gate = jnp.sum(jnp.where(same, gates, 0.0), axis=0, keepdims=True)
        hits = jnp.where(row_n == k, hit, hits)
        level = jnp.where(row_n == k, gate, level)
    before = (iota((rows, rows), 0) < iota((rows, rows), 1)).astype(BF16)
    rank = mm(hits.astype(BF16), before)
    place = jnp.where(hits > 0.5, rank, 1e4)
    sub = iota((PIECE, rows), 0)
    slot = jnp.where(sub >= CAP, sub - CAP, sub).astype(F32)
    firsts, seconds, scales = [], [], []
    for k in range(n):
        chosen = place[k : k + 1, :] == slot
        firsts.append(jnp.where(chosen & (sub < CAP), 1.0, 0.0))
        seconds.append(jnp.where(chosen & (sub >= CAP), 1.0, 0.0))
        scales.append(jnp.sum(jnp.where(chosen, level[k : k + 1, :], 0.0), axis=1, keepdims=True))
    first = jnp.concatenate(firsts, axis=0).astype(BF16)
    second = jnp.concatenate(seconds, axis=0).astype(BF16)
    scale = jnp.concatenate(scales, axis=0)
    pick_ref[0] = first
    pick_ref[1] = second
    half = width // FOLD
    chunk = min(512, half)
    for c in range(0, half, chunk):
        picked = mm(first, up_ref[:, c : c + chunk]) + mm(second, up_ref[:, half + c : half + c + chunk])
        picked = (picked * scale).astype(BF16)
        for k in range(2):
            blocks[k][:, c : c + chunk] = picked[k * PIECE : (k + 1) * PIECE]
        for m in range(1, n // 2):
            blocks[m + 1][:, c : c + chunk] = picked[2 * m * PIECE : 2 * (m + 1) * PIECE]


def route(me, trainable, ids, gates, upstream):
    n = trainable.shape[0]
    rows, width = upstream.shape
    half = width // FOLD
    out_shape = [jax.ShapeDtypeStruct((2, n * PIECE, rows), BF16)] + [
        jax.ShapeDtypeStruct((PIECE if m < 2 else 2 * PIECE, half), BF16) for m in range(n // 2 + 1)
    ]
    outs = pl.pallas_call(
        lambda *refs: route_kernel(n, rows, width, *refs),
        out_shape=out_shape,
        in_specs=[SMEM_SPEC, SMEM_SPEC] + [pl.BlockSpec(memory_space=pltpu.VMEM)] * 3,
        compiler_params=params(),
        cost_estimate=pl.CostEstimate(flops=4 * 10**9, bytes_accessed=2 * 10**6, transcendentals=0),
        name="route",
    )(me, trainable, ids, gates, upstream)
    return outs[0], list(outs[1:])


def unfold(pieces, out_ref):
    n = len(pieces)
    slots, width = out_ref.shape
    half = width // FOLD
    r = iota((slots, n * PIECE), 0)
    s = iota((slots, n * PIECE), 1)
    start = r
    for k in range(1, n):
        start = start + jnp.where(r >= k * CAP, PIECE - CAP, 0)
    chunk = min(512, half)
    for f in range(FOLD):
        select = (s == start + f * CAP).astype(BF16)
        for c in range(0, half, chunk):
            stacked = jnp.concatenate([ref[at : at + PIECE, c : c + chunk] for ref, at in pieces], axis=0)
            at = f * half + c
            out_ref[:, at : at + chunk] = mm(select, stacked).astype(BF16)


def forward_kernel(n, rows, width, me_ref, span_ref, *refs):
    kv_refs = refs[:n]
    q_ref, pick_ref, gain_ref = refs[n : n + 3]
    ka_ref, va_ref, kt_ref, vt_ref, exp_ref, inv_ref, mixed_ref, factor_ref = refs[n + 3 : n + 11]
    blocks = refs[n + 11 : n + 11 + n]
    b_ref, all_ref = refs[n + 11 + n :]
    step = pl.program_id(0)
    half_rows = rows // 2
    per_step = STEP_HEADS * HEAD_SIZE
    groups = ka_ref.shape[0]

    @pl.when(step == 0)
    def _():
        me = me_ref[0]
        lane = iota((rows, rows), 1)
        sub = iota((rows, rows), 0)
        lane_half = (lane >= half_rows).astype(jnp.int32)
        sub_half = (sub >= half_rows).astype(jnp.int32)
        lane_in = lane - lane_half * half_rows
        sub_in = sub - sub_half * half_rows
        b_ref[...] = jnp.where((lane_half == sub_half) & (lane_in >= sub_in), MASK_FILLER, 0.0).astype(BF16)
        mine0 = span_ref[0, 2 * me]
        mine1 = span_ref[0, 2 * me + 1]
        lane_span = jnp.where(lane_half == 0, mine0, mine1)
        for b in range(n):
            source = peer_of(me, b, n, -1)
            sub_span = jnp.where(sub_half == 0, span_ref[0, 2 * source], span_ref[0, 2 * source + 1])
            hot = ((sub_span == lane_span) & (lane_in == sub_in - 1)) | (
                (sub_span > lane_span) & (lane_in == half_rows - 1)
            )
            hot = jnp.where(hot, 1.0, 0.0).astype(BF16)
            kv = kv_refs[b][...]
            at = slice(b * rows, (b + 1) * rows)
            for g in range(groups):
                key = kv[:, g * HEAD_SIZE : (g + 1) * HEAD_SIZE]
                value = kv[:, (groups + g) * HEAD_SIZE : (groups + g + 1) * HEAD_SIZE]
                ka_ref[g, at, :HEAD_SIZE] = key
                ka_ref[g, at, HEAD_SIZE:] = hot
                va_ref[g, at, :HEAD_SIZE] = value
                va_ref[g, at, HEAD_SIZE:] = jnp.full((rows, HEAD_SIZE), -1.0, BF16)
                kt_ref[g, :, at] = key.T
                vt_ref[g, :HEAD_SIZE, at] = value.T
                vt_ref[g, HEAD_SIZE:, at] = jnp.ones((16, rows), BF16)

    g = step // (HEADS_PER_GROUP // STEP_HEADS)
    b = b_ref[...]

    def paired(p):
        at = p * 2 * HEAD_SIZE
        q0 = q_ref[:, at : at + HEAD_SIZE]
        q1 = q_ref[:, at + HEAD_SIZE : at + 2 * HEAD_SIZE]
        return jnp.concatenate(
            [jnp.concatenate([q0, b], axis=1), jnp.concatenate([q1, b], axis=1)], axis=0
        )

    ahead = mm_t(ka_ref[g], paired(0))
    for p in range(STEP_HEADS // 2):
        at = p * 2 * HEAD_SIZE
        scores = ahead
        if p + 1 < STEP_HEADS // 2:
            ahead = mm_t(ka_ref[g], paired(p + 1))
        peak = jnp.max(scores, axis=0, keepdims=True)
        exps = jnp.exp2((scores - peak) * (SCALE * LOG2E)).astype(BF16)
        exp_ref[p] = exps
        out = mm(vt_ref[g], exps)
        inv = 1.0 / out[HEAD_SIZE : HEAD_SIZE + 1, :]
        normal = out[:HEAD_SIZE, :] * inv
        inv_full = jnp.broadcast_to(inv, (rows, 2 * rows))
        for i in range(2):
            cols = slice(at + i * HEAD_SIZE, at + (i + 1) * HEAD_SIZE)
            head = normal[:, i * rows : (i + 1) * rows].T.astype(BF16)
            mixed_ref[:, cols] = head
            all_ref[step, :, cols] = head
            inv_ref[:, cols] = inv_full[:, i * rows : (i + 1) * rows].T

    @pl.when(step == pl.num_programs(0) - 1)
    def _():
        steps = width // per_step
        square = jnp.zeros((rows, 1), F32)
        for i in range(steps):
            part = all_ref[i].astype(F32)
            square = square + jnp.sum(part * part, axis=1, keepdims=True)
        factor = lax.rsqrt(square / width + EPSILON)
        factor_ref[...] = jnp.broadcast_to(factor, (rows, 128))

        def normed(i):
            gain = gain_ref[:, i * per_step : (i + 1) * per_step]
            return (all_ref[i].astype(F32) * factor * gain).astype(BF16)

        for i in range(steps // FOLD):
            picked = mm(pick_ref[0], normed(i)) + mm(pick_ref[1], normed(steps // FOLD + i))
            picked = picked.astype(BF16)
            for k in range(n):
                blocks[k][:, i * per_step : (i + 1) * per_step] = picked[k * PIECE : (k + 1) * PIECE]


def forward(me, span, kv_blocks, query, pick, gain):
    n = len(kv_blocks)
    rows, width = query.shape
    groups = kv_blocks[0].shape[1] // (2 * HEAD_SIZE)
    total = n * rows
    per_step = STEP_HEADS * HEAD_SIZE
    steps = width // per_step
    half = width // FOLD
    pairs = width // (2 * HEAD_SIZE)
    out_shape = [
        jax.ShapeDtypeStruct((groups, total, 2 * HEAD_SIZE), BF16),
        jax.ShapeDtypeStruct((groups, total, 2 * HEAD_SIZE), BF16),
        jax.ShapeDtypeStruct((groups, HEAD_SIZE, total), BF16),
        jax.ShapeDtypeStruct((groups, HEAD_SIZE + 16, total), BF16),
        jax.ShapeDtypeStruct((pairs, total, 2 * rows), BF16),
        jax.ShapeDtypeStruct((rows, width), F32),
        jax.ShapeDtypeStruct((rows, width), BF16),
        jax.ShapeDtypeStruct((rows, 128), F32),
    ] + [jax.ShapeDtypeStruct((PIECE, half), BF16) for _ in range(n)]
    column = pl.BlockSpec((rows, per_step), lambda i: (0, i))
    out_specs = [whole(s.shape) for s in out_shape]
    out_specs[4] = pl.BlockSpec((STEP_HEADS // 2, total, 2 * rows), lambda i: (i, 0, 0))
    out_specs[5] = column
    out_specs[6] = column
    outs = pl.pallas_call(
        lambda *refs: forward_kernel(n, rows, width, *refs),
        out_shape=out_shape,
        grid=(steps,),
        in_specs=[SMEM_SPEC, SMEM_SPEC]
        + [whole(kv_blocks[0].shape)] * n
        + [column, whole(pick.shape), whole(gain.shape)],
        out_specs=out_specs,
        scratch_shapes=[pltpu.VMEM((rows, rows), BF16), pltpu.VMEM((steps, rows, per_step), BF16)],
        compiler_params=params("arbitrary"),
        cost_estimate=pl.CostEstimate(flops=10**10, bytes_accessed=2 * 10**7, transcendentals=4 * 10**6),
        name="forward",
    )(me, span, *kv_blocks, query, pick, gain)
    return outs[:8], list(outs[8:])


def gated(gate_in, up_in, back):
    sigma = 1.0 / (1.0 + jnp.exp(-gate_in))
    act = gate_in * sigma
    grad_gate = (back * up_in * sigma * (1.0 + gate_in * (1.0 - sigma))).astype(BF16)
    grad_up = (back * act).astype(BF16)
    product = (act * up_in).astype(BF16)
    return grad_gate, grad_up, product


def early_kernel(n, *refs):
    blocks, (weights, rows_ref, back_ref) = refs[:n], refs[n:]

    @pl.when(pl.program_id(0) == 0)
    def _():
        unfold([(ref, PIECE if b > 2 and b % 2 else 0) for b, ref in enumerate(blocks)], rows_ref)

    back_ref[...] = mm_t(rows_ref[...], weights[0])


def early(blocks, weights):
    n = len(blocks)
    hidden, width = weights.shape[1:]
    slots = n * CAP
    tile = 256
    return pl.pallas_call(
        lambda *refs: early_kernel(n, *refs),
        out_shape=[jax.ShapeDtypeStruct((slots, width), BF16), jax.ShapeDtypeStruct((slots, hidden), F32)],
        grid=(hidden // tile,),
        in_specs=[whole(b.shape) for b in blocks] + [pl.BlockSpec((1, tile, width), lambda i: (2, i, 0))],
        out_specs=[whole((slots, width)), pl.BlockSpec((slots, tile), lambda i: (0, i))],
        compiler_params=params("arbitrary"),
        cost_estimate=pl.CostEstimate(flops=2 * 10**9, bytes_accessed=7 * 10**6, transcendentals=0),
        name="early",
    )(*blocks, weights)


def expert_kernel(n, slots, *refs):
    arrived, (back_ref, weights, routed_ref), blocks, acc_ref = refs[:n], refs[n : n + 3], refs[n + 3 : -1], refs[-1]
    step = pl.program_id(0)
    width = acc_ref.shape[1]

    @pl.when(step == 0)
    def _():
        unfold([(ref, 0) for ref in arrived], routed_ref)

    routed = routed_ref[...]
    gate_in = mm_t(routed, weights[0])
    up_in = mm_t(routed, weights[1])
    grad_gate, grad_up, _ = gated(gate_in, up_in, back_ref[...])
    got = mm(grad_gate, weights[0]) + mm(grad_up, weights[1])

    @pl.when(step == 0)
    def _():
        acc_ref[...] = got

    @pl.when(step > 0)
    def _():
        acc_ref[...] += got

    @pl.when(step == pl.num_programs(0) - 1)
    def _():
        half = width // FOLD
        r = iota((n * PIECE, slots), 1)
        s = iota((n * PIECE, slots), 0)
        start = r
        for k in range(1, n):
            start = start + jnp.where(r >= k * CAP, PIECE - CAP, 0)
        first = (s == start).astype(BF16)
        second = (s == start + CAP).astype(BF16)
        chunk = min(512, half)
        for c in range(0, half, chunk):
            spread = mm(first, acc_ref[:, c : c + chunk].astype(BF16)) + mm(
                second, acc_ref[:, half + c : half + c + chunk].astype(BF16)
            )
            spread = spread.astype(BF16)
            for k in range(n):
                blocks[k][:, c : c + chunk] = spread[k * PIECE : (k + 1) * PIECE]


def expert(arrived, back, weights):
    n = len(arrived)
    slots = n * CAP
    hidden, width = weights.shape[1:]
    tile = 256
    half = width // FOLD
    outs = pl.pallas_call(
        lambda *refs: expert_kernel(n, slots, *refs),
        out_shape=[jax.ShapeDtypeStruct((slots, width), BF16)] + [jax.ShapeDtypeStruct((PIECE, half), BF16)] * n,
        grid=(hidden // tile,),
        in_specs=[whole(b.shape) for b in arrived]
        + [
            pl.BlockSpec((slots, tile), lambda i: (0, i)),
            pl.BlockSpec((2, tile, width), lambda i: (0, i, 0)),
        ],
        out_specs=[whole((slots, width))] + [whole((PIECE, half))] * n,
        scratch_shapes=[pltpu.VMEM((slots, width), F32)],
        compiler_params=params("arbitrary"),
        cost_estimate=pl.CostEstimate(flops=8 * 10**9, bytes_accessed=2 * 10**7, transcendentals=0),
        name="expert",
    )(*arrived, back, weights)
    return outs[0], list(outs[1:])


def grads_kernel(count, share, dp_ref, *refs):
    row_parts, grad_parts = refs[:count], refs[count : 2 * count]
    weights, out_ref, rows_ref, grads_ref, w_ref, side_ref, sems = refs[2 * count :]
    part = row_parts[0].shape[0]
    chunk = out_ref.shape[2]

    @pl.when(pl.program_id(0) == 0)
    def _():
        first = pl.multiple_of(dp_ref[0] * share, 32)
        copies = []
        for i in range(3):
            source = weights.at[i, pl.ds(first, share)]
            copies.append(pltpu.make_async_copy(source, w_ref.at[i], sems.at[2 * count + i]))
        late = [copies.pop()]
        for i in range(count):
            at = pl.ds(i * part, part)
            copies.append(pltpu.make_async_copy(row_parts[i], rows_ref.at[at], sems.at[i]))
            late.append(pltpu.make_async_copy(grad_parts[i], grads_ref.at[at], sems.at[count + i]))
        for copy in copies + late:
            copy.start()
        for copy in copies:
            copy.wait()
        rows = rows_ref[...]
        gate_in = mm_t(rows, w_ref[0])
        up_in = mm_t(rows, w_ref[1])
        for copy in late:
            copy.wait()
        back = mm_t(grads_ref[...], w_ref[2])
        for i, side in enumerate(gated(gate_in, up_in, back)):
            side_ref[i] = side

    at = pl.ds(pl.multiple_of(pl.program_id(0) * chunk, chunk), chunk)
    out_ref[0] = t_mm(side_ref[0], rows_ref[:, at]).astype(BF16)
    out_ref[1] = t_mm(side_ref[1], rows_ref[:, at]).astype(BF16)
    out_ref[2] = t_mm(side_ref[2], grads_ref[:, at]).astype(BF16)


def expert_gradients(dp_index, row_parts, grad_parts, weights, share):
    count = len(row_parts)
    width = weights.shape[2]
    slots = row_parts[0].shape[0]
    total = count * slots
    chunk = width // 4
    anywhere = pl.BlockSpec(memory_space=pl.ANY)
    return pl.pallas_call(
        lambda *refs: grads_kernel(count, share, *refs),
        out_shape=jax.ShapeDtypeStruct((3, share, width), BF16),
        grid=(width // chunk,),
        in_specs=[SMEM_SPEC] + [anywhere] * (2 * count + 1),
        out_specs=pl.BlockSpec((3, share, chunk), lambda i: (0, 0, i)),
        scratch_shapes=[
            pltpu.VMEM((total, width), BF16),
            pltpu.VMEM((total, width), BF16),
            pltpu.VMEM((3, share, width), BF16),
            pltpu.VMEM((3, total, share), BF16),
            pltpu.SemaphoreType.DMA((2 * count + 3,)),
        ],
        compiler_params=params("arbitrary"),
        cost_estimate=pl.CostEstimate(flops=10**10, bytes_accessed=15 * 10**6, transcendentals=0),
        name="grads",
    )(dp_index, *row_parts, *grad_parts, weights)


def backward_kernel(n, rows, width, *refs):
    back_refs = refs[:n]
    pick_ref, up_ref, mixed_ref, gain_ref, factor_ref, q_ref, inv_ref, exp_ref, va_ref, kt_ref = refs[n : n + 10]
    dq_ref, near_ref, far_ref = refs[n + 10 : n + 13]
    gm_ref, ig_ref, dk_ref, dv_ref = refs[n + 13 :]
    step = pl.program_id(0)
    per_step = STEP_HEADS * HEAD_SIZE
    per_group = HEADS_PER_GROUP // STEP_HEADS
    chunks = width // per_step
    g = step // per_group

    @pl.when(step == 0)
    def _():
        half_chunks = chunks // FOLD
        total = jnp.zeros((rows, 1), F32)
        for i in range(chunks):
            f, c = i // half_chunks, (i % half_chunks) * per_step
            stacked = jnp.concatenate([b[:, c : c + per_step] for b in back_refs], axis=0)
            grad = t_mm(pick_ref[f], stacked) * gain_ref[:, i * per_step : (i + 1) * per_step]
            ig_ref[i] = grad
            mixed = mixed_ref[:, i * per_step : (i + 1) * per_step].astype(F32)
            total = total + jnp.sum(grad * mixed, axis=1, keepdims=True)
        factor = factor_ref[:, :1]
        pull = factor * factor * factor * (total / width)
        for i in range(chunks):
            mixed = mixed_ref[:, i * per_step : (i + 1) * per_step].astype(F32)
            up = up_ref[:, i * per_step : (i + 1) * per_step].astype(F32)
            gm_ref[i] = (up + (factor * ig_ref[i] - mixed * pull)).astype(BF16)

    @pl.when(step % per_group == 0)
    def _():
        dk_ref[...] = jnp.zeros_like(dk_ref)
        dv_ref[...] = jnp.zeros_like(dv_ref)

    col = pl.multiple_of(step * per_step, per_step)
    grad_all = gm_ref[step].astype(F32) * inv_ref[...]
    grad_b = grad_all.astype(BF16)
    prod = (grad_b.astype(F32) * mixed_ref[:, pl.ds(col, per_step)].astype(F32)).astype(BF16)

    def stack(x, p):
        at = p * 2 * HEAD_SIZE
        return jnp.concatenate([x[:, at : at + HEAD_SIZE], x[:, at + HEAD_SIZE : at + 2 * HEAD_SIZE]], axis=0)

    def push(p):
        return mm_t(va_ref[g], jnp.concatenate([stack(grad_b, p), stack(prod, p)], axis=1))

    ahead = push(0)
    for p in range(STEP_HEADS // 2):
        at = p * 2 * HEAD_SIZE
        gs = stack(grad_b, p)
        pushed = ahead
        if p + 1 < STEP_HEADS // 2:
            ahead = push(p + 1)
        exps = exp_ref[p]
        slopes = (exps.astype(F32) * pushed).astype(BF16)
        qs = jnp.concatenate([q_ref[:, at : at + HEAD_SIZE], q_ref[:, at + HEAD_SIZE : at + 2 * HEAD_SIZE]], axis=0)
        dk_ref[...] += mm(slopes, qs)
        dv_ref[...] += mm(exps, gs)
        dq = mm(kt_ref[g], slopes) * SCALE
        for i in range(2):
            cols = slice(at + i * HEAD_SIZE, at + (i + 1) * HEAD_SIZE)
            dq_ref[:, cols] = dq[:, i * rows : (i + 1) * rows].T.astype(BF16)

    groups = va_ref.shape[0]
    for gg in range(groups):

        @pl.when(step == (gg + 1) * per_group - 1)
        def _():
            for b in range(n):
                at = slice(b * rows, (b + 1) * rows)
                kcol = slice(gg * HEAD_SIZE, (gg + 1) * HEAD_SIZE)
                vcol = slice((groups + gg) * HEAD_SIZE, (groups + gg + 1) * HEAD_SIZE)
                if b % 2 == 0:
                    near_ref[b // 2, :, kcol] = dk_ref[at] * SCALE
                    near_ref[b // 2, :, vcol] = dv_ref[at]
                else:
                    far_ref[b // 2, :, kcol] = (dk_ref[at] * SCALE).astype(BF16)
                    far_ref[b // 2, :, vcol] = dv_ref[at].astype(BF16)


def backward(back, pick, upstream, gain, query, fwd):
    _, va, kt, _, exps, inv, mixed, factor = fwd
    n = len(back)
    rows, width = query.shape
    groups, total = va.shape[:2]
    per_step = STEP_HEADS * HEAD_SIZE
    steps = width // per_step
    column = pl.BlockSpec((rows, per_step), lambda i: (0, i))
    kv_width = 2 * groups * HEAD_SIZE
    return pl.pallas_call(
        lambda *refs: backward_kernel(n, rows, width, *refs),
        out_shape=[
            jax.ShapeDtypeStruct((rows, width), BF16),
            jax.ShapeDtypeStruct((n // 2, rows, kv_width), F32),
            jax.ShapeDtypeStruct((n // 2, rows, kv_width), BF16),
        ],
        grid=(steps,),
        in_specs=[whole(back[0].shape)] * n
        + [whole(pick.shape), whole(upstream.shape), whole(mixed.shape), whole(gain.shape), whole(factor.shape)]
        + [
            column,
            column,
            pl.BlockSpec((STEP_HEADS // 2, total, 2 * rows), lambda i: (i, 0, 0)),
            whole(va.shape),
            whole(kt.shape),
        ],
        out_specs=[column, whole((n // 2, rows, kv_width)), whole((n // 2, rows, kv_width))],
        scratch_shapes=[
            pltpu.VMEM((steps, rows, per_step), BF16),
            pltpu.VMEM((steps, rows, per_step), F32),
            pltpu.VMEM((total, HEAD_SIZE), F32),
            pltpu.VMEM((total, HEAD_SIZE), F32),
        ],
        compiler_params=params("arbitrary"),
        cost_estimate=pl.CostEstimate(flops=2 * 10**10, bytes_accessed=2 * 10**7, transcendentals=0),
        name="backward",
    )(*back, pick, upstream, mixed, gain, factor, query, inv, exps, va, kt)


def shift(x, axis, k):
    n = lax.axis_size(axis)
    return lax.ppermute(x, axis, [(i, (i + k) % n) for i in range(n)])


def flip(x, axis, bit):
    n = lax.axis_size(axis)
    return lax.ppermute(x, axis, [(i, i ^ bit) for i in range(n)])


def exchange(blocks, sign):
    n = len(blocks)
    got = [blocks[0]] + [None] * (n - 1)
    chips = n // 2
    for b in sorted(range(1, n), key=lambda b: -min(b // 2, chips - b // 2)):
        got[b] = lax.ppermute(blocks[b], "ctx", [(i, peer_of(i, b, n, sign)) for i in range(n)])
    return got


def gather_docs(rows):
    n = lax.axis_size("dp")
    return [rows] + [flip(rows, "dp", k) for k in range(n - 1, 0, -1)]


def per_device(
    query,
    key,
    value,
    span_order,
    expert_ids,
    expert_gates,
    trainable,
    norm_gain,
    upstream,
    expert_weights,
):
    n = lax.axis_size("ctx")
    chips = n // 2
    me = lax.axis_index("ctx").astype(jnp.int32).reshape(1)
    dp_index = lax.axis_index("dp").astype(jnp.int32).reshape(1)
    weights = expert_weights[0].transpose(1, 0, 2)
    gain = norm_gain[None, :]
    grad_out = upstream[0]

    kv = jnp.concatenate([key[0], value[0]], axis=1)
    arrived = [kv] + [shift(kv, "ctx", 2 * m) for m in range(1, chips)]
    kv_blocks = []
    for block in arrived:
        kv_blocks += [block, flip(block, "ctx", 1)]

    pick, grad_blocks = route(me, trainable, expert_ids[0].T, expert_gates[0].T, grad_out)
    pairs = [shift(grad_blocks[m + 1], "ctx", 2 * m) for m in range(1, chips)]
    grad_blocks = [grad_blocks[0], flip(grad_blocks[1], "ctx", 1)]
    for pair in pairs:
        grad_blocks += [pair, flip(pair, "ctx", 1)]
    weighted, back_rows = early(grad_blocks, weights)
    all_weighted = gather_docs(weighted)

    fwd, row_blocks = forward(me, span_order, kv_blocks, query[0], pick, gain)
    row_blocks = exchange(row_blocks, 1)
    routed, returned = expert(row_blocks, back_rows, weights)
    all_routed = gather_docs(routed)
    back = exchange(returned, -1)
    share = weights.shape[1] // lax.axis_size("dp")
    expert_grads = expert_gradients(dp_index, all_routed, all_weighted, weights, share)
    d_query, near, far = backward(back, pick, grad_out, gain, query[0], fwd)

    far = flip(far, "ctx", 1)
    met = near + far.astype(F32)
    total = met[0]
    sent = met.astype(BF16)
    landed = [shift(sent[m], "ctx", -2 * m) for m in range(1, chips)]
    for block in landed:
        total = total + block.astype(F32)
    split = key.shape[2]
    return (
        d_query[None],
        total[:, :split].astype(BF16)[None],
        total[:, split:].astype(BF16)[None],
        expert_grads.transpose(1, 0, 2)[None],
    )


def solution(mesh):
    in_specs = (
        P("dp", "ctx", None),
        P("dp", "ctx", None),
        P("dp", "ctx", None),
        P("dp", None),
        P("dp", "ctx", None),
        P("dp", "ctx", None),
        P(),
        P(),
        P("dp", "ctx", None),
        P("ctx", None, None, None),
    )
    out_specs = (
        P("dp", "ctx", None),
        P("dp", "ctx", None),
        P("dp", "ctx", None),
        P("ctx", "dp", None, None),
    )

    return jax.shard_map(per_device, mesh=mesh, in_specs=in_specs, out_specs=out_specs, check_vma=False)
```

```python
import jax
import jax.numpy as jnp
from jax import lax
from jax.experimental import pallas as pl
from jax.experimental.pallas import tpu as pltpu
from jax.sharding import PartitionSpec as P


HEADS_PER_GROUP = 16
HEAD_SIZE = 128
CAP = 12
EPSILON = 1e-06
MASK_FILLER = -1e30
SCALE = HEAD_SIZE ** (-0.5)
LOG2E = 1.4426950408889634
FOLD = 2
PIECE = FOLD * CAP
STEP_HEADS = 8
F32 = jnp.float32
BF16 = jnp.bfloat16


def mm(a, b):
    return lax.dot_general(a, b, (((1,), (0,)), ((), ())), preferred_element_type=F32)


def mm_t(a, b):
    return lax.dot_general(a, b, (((1,), (1,)), ((), ())), preferred_element_type=F32)


def t_mm(a, b):
    return lax.dot_general(a, b, (((0,), (0,)), ((), ())), preferred_element_type=F32)


def iota(shape, dim):
    return lax.broadcasted_iota(jnp.int32, shape, dim)


def params(*semantics):
    if semantics:
        return pltpu.CompilerParams(dimension_semantics=semantics, vmem_limit_bytes=60 << 20)
    return pltpu.CompilerParams(vmem_limit_bytes=60 << 20)


def whole(shape):
    return pl.BlockSpec(shape, lambda *_: (0,) * len(shape))


SMEM_SPEC = pl.BlockSpec(memory_space=pltpu.SMEM)


def peer_of(me, b, n, sign):
    core = me % 2
    chip = (me // 2 + sign * (b // 2) + n // 2) % (n // 2)
    return 2 * chip + (core if b % 2 == 0 else 1 - core)


def route_kernel(n, rows, width, me_ref, train_ref, ids_ref, gates_ref, up_ref, *outs):
    pick_ref, blocks = outs[0], outs[1:]
    ids = ids_ref[...]
    gates = gates_ref[...]
    me = me_ref[0]
    row_n = iota((n, rows), 0)
    hits = jnp.zeros((n, rows), F32)
    level = jnp.zeros((n, rows), F32)
    for k in range(n):
        same = ids == train_ref[peer_of(me, k, n, 1)]
        hit = jnp.sum(same.astype(F32), axis=0, keepdims=True)
        gate = jnp.sum(jnp.where(same, gates, 0.0), axis=0, keepdims=True)
        hits = jnp.where(row_n == k, hit, hits)
        level = jnp.where(row_n == k, gate, level)
    before = (iota((rows, rows), 0) < iota((rows, rows), 1)).astype(BF16)
    rank = mm(hits.astype(BF16), before)
    place = jnp.where(hits > 0.5, rank, 1e4)
    sub = iota((PIECE, rows), 0)
    slot = jnp.where(sub >= CAP, sub - CAP, sub).astype(F32)
    firsts, seconds, scales = [], [], []
    for k in range(n):
        chosen = place[k : k + 1, :] == slot
        firsts.append(jnp.where(chosen & (sub < CAP), 1.0, 0.0))
        seconds.append(jnp.where(chosen & (sub >= CAP), 1.0, 0.0))
        scales.append(jnp.sum(jnp.where(chosen, level[k : k + 1, :], 0.0), axis=1, keepdims=True))
    first = jnp.concatenate(firsts, axis=0).astype(BF16)
    second = jnp.concatenate(seconds, axis=0).astype(BF16)
    scale = jnp.concatenate(scales, axis=0)
    pick_ref[0] = first
    pick_ref[1] = second
    half = width // FOLD
    chunk = min(512, half)
    for c in range(0, half, chunk):
        picked = mm(first, up_ref[:, c : c + chunk]) + mm(second, up_ref[:, half + c : half + c + chunk])
        picked = (picked * scale).astype(BF16)
        for k in range(2):
            blocks[k][:, c : c + chunk] = picked[k * PIECE : (k + 1) * PIECE]
        for m in range(1, n // 2):
            blocks[m + 1][:, c : c + chunk] = picked[2 * m * PIECE : 2 * (m + 1) * PIECE]


def route(me, trainable, ids, gates, upstream):
    n = trainable.shape[0]
    rows, width = upstream.shape
    half = width // FOLD
    out_shape = [jax.ShapeDtypeStruct((2, n * PIECE, rows), BF16)] + [
        jax.ShapeDtypeStruct((PIECE if m < 2 else 2 * PIECE, half), BF16) for m in range(n // 2 + 1)
    ]
    outs = pl.pallas_call(
        lambda *refs: route_kernel(n, rows, width, *refs),
        out_shape=out_shape,
        in_specs=[SMEM_SPEC, SMEM_SPEC] + [pl.BlockSpec(memory_space=pltpu.VMEM)] * 3,
        compiler_params=params(),
        cost_estimate=pl.CostEstimate(flops=4 * 10**9, bytes_accessed=2 * 10**6, transcendentals=0),
        name="route",
    )(me, trainable, ids, gates, upstream)
    return outs[0], list(outs[1:])


def unfold(pieces, out_ref):
    n = len(pieces)
    slots, width = out_ref.shape
    half = width // FOLD
    r = iota((slots, n * PIECE), 0)
    s = iota((slots, n * PIECE), 1)
    start = r
    for k in range(1, n):
        start = start + jnp.where(r >= k * CAP, PIECE - CAP, 0)
    chunk = min(512, half)
    for f in range(FOLD):
        select = (s == start + f * CAP).astype(BF16)
        for c in range(0, half, chunk):
            stacked = jnp.concatenate([ref[at : at + PIECE, c : c + chunk] for ref, at in pieces], axis=0)
            at = f * half + c
            out_ref[:, at : at + chunk] = mm(select, stacked).astype(BF16)


def forward_kernel(n, rows, width, me_ref, span_ref, *refs):
    kv_refs = refs[:n]
    q_ref, pick_ref, gain_ref = refs[n : n + 3]
    ka_ref, va_ref, kt_ref, vt_ref, exp_ref, inv_ref, mixed_ref, factor_ref = refs[n + 3 : n + 11]
    blocks = refs[n + 11 : n + 11 + n]
    b_ref, all_ref = refs[n + 11 + n :]
    step = pl.program_id(0)
    half_rows = rows // 2
    per_step = STEP_HEADS * HEAD_SIZE
    groups = ka_ref.shape[0]

    @pl.when(step == 0)
    def _():
        me = me_ref[0]
        lane = iota((rows, rows), 1)
        sub = iota((rows, rows), 0)
        lane_half = (lane >= half_rows).astype(jnp.int32)
        sub_half = (sub >= half_rows).astype(jnp.int32)
        lane_in = lane - lane_half * half_rows
        sub_in = sub - sub_half * half_rows
        b_ref[...] = jnp.where((lane_half == sub_half) & (lane_in >= sub_in), MASK_FILLER, 0.0).astype(BF16)
        mine0 = span_ref[0, 2 * me]
        mine1 = span_ref[0, 2 * me + 1]
        lane_span = jnp.where(lane_half == 0, mine0, mine1)
        for b in range(n):
            source = peer_of(me, b, n, -1)
            sub_span = jnp.where(sub_half == 0, span_ref[0, 2 * source], span_ref[0, 2 * source + 1])
            hot = ((sub_span == lane_span) & (lane_in == sub_in - 1)) | (
                (sub_span > lane_span) & (lane_in == half_rows - 1)
            )
            hot = jnp.where(hot, 1.0, 0.0).astype(BF16)
            kv = kv_refs[b][...]
            at = slice(b * rows, (b + 1) * rows)
            for g in range(groups):
                key = kv[:, g * HEAD_SIZE : (g + 1) * HEAD_SIZE]
                value = kv[:, (groups + g) * HEAD_SIZE : (groups + g + 1) * HEAD_SIZE]
                ka_ref[g, at, :HEAD_SIZE] = key
                ka_ref[g, at, HEAD_SIZE:] = hot
                va_ref[g, at, :HEAD_SIZE] = value
                va_ref[g, at, HEAD_SIZE:] = jnp.full((rows, HEAD_SIZE), -1.0, BF16)
                kt_ref[g, :, at] = key.T
                vt_ref[g, :HEAD_SIZE, at] = value.T
                vt_ref[g, HEAD_SIZE:, at] = jnp.ones((16, rows), BF16)

    g = step // (HEADS_PER_GROUP // STEP_HEADS)
    b = b_ref[...]

    def paired(p):
        at = p * 2 * HEAD_SIZE
        q0 = q_ref[:, at : at + HEAD_SIZE]
        q1 = q_ref[:, at + HEAD_SIZE : at + 2 * HEAD_SIZE]
        return jnp.concatenate(
            [jnp.concatenate([q0, b], axis=1), jnp.concatenate([q1, b], axis=1)], axis=0
        )

    ahead = mm_t(ka_ref[g], paired(0))
    for p in range(STEP_HEADS // 2):
        at = p * 2 * HEAD_SIZE
        scores = ahead
        if p + 1 < STEP_HEADS // 2:
            ahead = mm_t(ka_ref[g], paired(p + 1))
        peak = jnp.max(scores, axis=0, keepdims=True)
        exps = jnp.exp2((scores - peak) * (SCALE * LOG2E)).astype(BF16)
        exp_ref[p] = exps
        out = mm(vt_ref[g], exps)
        inv = 1.0 / out[HEAD_SIZE : HEAD_SIZE + 1, :]
        normal = out[:HEAD_SIZE, :] * inv
        inv_full = jnp.broadcast_to(inv, (rows, 2 * rows))
        for i in range(2):
            cols = slice(at + i * HEAD_SIZE, at + (i + 1) * HEAD_SIZE)
            head = normal[:, i * rows : (i + 1) * rows].T.astype(BF16)
            mixed_ref[:, cols] = head
            all_ref[step, :, cols] = head
            inv_ref[:, cols] = inv_full[:, i * rows : (i + 1) * rows].T

    @pl.when(step == pl.num_programs(0) - 1)
    def _():
        steps = width // per_step
        square = jnp.zeros((rows, 1), F32)
        for i in range(steps):
            part = all_ref[i].astype(F32)
            square = square + jnp.sum(part * part, axis=1, keepdims=True)
        factor = lax.rsqrt(square / width + EPSILON)
        factor_ref[...] = jnp.broadcast_to(factor, (rows, 128))

        def normed(i):
            gain = gain_ref[:, i * per_step : (i + 1) * per_step]
            return (all_ref[i].astype(F32) * factor * gain).astype(BF16)

        for i in range(steps // FOLD):
            picked = mm(pick_ref[0], normed(i)) + mm(pick_ref[1], normed(steps // FOLD + i))
            picked = picked.astype(BF16)
            for k in range(n):
                blocks[k][:, i * per_step : (i + 1) * per_step] = picked[k * PIECE : (k + 1) * PIECE]


def forward(me, span, kv_blocks, query, pick, gain):
    n = len(kv_blocks)
    rows, width = query.shape
    groups = kv_blocks[0].shape[1] // (2 * HEAD_SIZE)
    total = n * rows
    per_step = STEP_HEADS * HEAD_SIZE
    steps = width // per_step
    half = width // FOLD
    pairs = width // (2 * HEAD_SIZE)
    out_shape = [
        jax.ShapeDtypeStruct((groups, total, 2 * HEAD_SIZE), BF16),
        jax.ShapeDtypeStruct((groups, total, 2 * HEAD_SIZE), BF16),
        jax.ShapeDtypeStruct((groups, HEAD_SIZE, total), BF16),
        jax.ShapeDtypeStruct((groups, HEAD_SIZE + 16, total), BF16),
        jax.ShapeDtypeStruct((pairs, total, 2 * rows), BF16),
        jax.ShapeDtypeStruct((rows, width), F32),
        jax.ShapeDtypeStruct((rows, width), BF16),
        jax.ShapeDtypeStruct((rows, 128), F32),
    ] + [jax.ShapeDtypeStruct((PIECE, half), BF16) for _ in range(n)]
    column = pl.BlockSpec((rows, per_step), lambda i: (0, i))
    out_specs = [whole(s.shape) for s in out_shape]
    out_specs[4] = pl.BlockSpec((STEP_HEADS // 2, total, 2 * rows), lambda i: (i, 0, 0))
    out_specs[5] = column
    out_specs[6] = column
    outs = pl.pallas_call(
        lambda *refs: forward_kernel(n, rows, width, *refs),
        out_shape=out_shape,
        grid=(steps,),
        in_specs=[SMEM_SPEC, SMEM_SPEC]
        + [whole(kv_blocks[0].shape)] * n
        + [column, whole(pick.shape), whole(gain.shape)],
        out_specs=out_specs,
        scratch_shapes=[pltpu.VMEM((rows, rows), BF16), pltpu.VMEM((steps, rows, per_step), BF16)],
        compiler_params=params("arbitrary"),
        cost_estimate=pl.CostEstimate(flops=10**10, bytes_accessed=2 * 10**7, transcendentals=4 * 10**6),
        name="forward",
    )(me, span, *kv_blocks, query, pick, gain)
    return outs[:8], list(outs[8:])


def gated(gate_in, up_in, back):
    sigma = 1.0 / (1.0 + jnp.exp(-gate_in))
    act = gate_in * sigma
    grad_gate = (back * up_in * sigma * (1.0 + gate_in * (1.0 - sigma))).astype(BF16)
    grad_up = (back * act).astype(BF16)
    product = (act * up_in).astype(BF16)
    return grad_gate, grad_up, product


def split_rows(rows_ref, halves):
    part = halves[0].shape[0]
    for i, half in enumerate(halves):
        half[...] = rows_ref[i * part : (i + 1) * part]


def early_kernel(n, *refs):
    blocks, (weights, *halves, back_ref, rows_ref) = refs[:n], refs[n:]

    @pl.when(pl.program_id(0) == 0)
    def _():
        unfold([(ref, PIECE if b > 2 and b % 2 else 0) for b, ref in enumerate(blocks)], rows_ref)
        split_rows(rows_ref, halves)

    back_ref[...] = mm_t(rows_ref[...], weights[0])


def early(blocks, weights):
    n = len(blocks)
    hidden, width = weights.shape[1:]
    slots = n * CAP
    tile = 256
    return pl.pallas_call(
        lambda *refs: early_kernel(n, *refs),
        out_shape=[jax.ShapeDtypeStruct((slots // 2, width), BF16)] * 2
        + [jax.ShapeDtypeStruct((slots, hidden), F32)],
        grid=(hidden // tile,),
        scratch_shapes=[pltpu.VMEM((slots, width), BF16)],
        in_specs=[whole(b.shape) for b in blocks] + [pl.BlockSpec((1, tile, width), lambda i: (2, i, 0))],
        out_specs=[whole((slots // 2, width))] * 2 + [pl.BlockSpec((slots, tile), lambda i: (0, i))],
        compiler_params=params("arbitrary"),
        cost_estimate=pl.CostEstimate(flops=2 * 10**9, bytes_accessed=7 * 10**6, transcendentals=0),
        name="early",
    )(*blocks, weights)


def expert_kernel(n, slots, *refs):
    arrived, (back_ref, weights, *halves) = refs[:n], refs[n : n + 4]
    blocks, (acc_ref, routed_ref) = refs[n + 4 : -2], refs[-2:]
    step = pl.program_id(0)
    width = acc_ref.shape[1]

    @pl.when(step == 0)
    def _():
        unfold([(ref, 0) for ref in arrived], routed_ref)
        split_rows(routed_ref, halves)

    routed = routed_ref[...]
    gate_in = mm_t(routed, weights[0])
    up_in = mm_t(routed, weights[1])
    grad_gate, grad_up, _ = gated(gate_in, up_in, back_ref[...])
    got = mm(grad_gate, weights[0]) + mm(grad_up, weights[1])

    @pl.when(step == 0)
    def _():
        acc_ref[...] = got

    @pl.when(step > 0)
    def _():
        acc_ref[...] += got

    @pl.when(step == pl.num_programs(0) - 1)
    def _():
        half = width // FOLD
        r = iota((n * PIECE, slots), 1)
        s = iota((n * PIECE, slots), 0)
        start = r
        for k in range(1, n):
            start = start + jnp.where(r >= k * CAP, PIECE - CAP, 0)
        first = (s == start).astype(BF16)
        second = (s == start + CAP).astype(BF16)
        chunk = min(512, half)
        for c in range(0, half, chunk):
            spread = mm(first, acc_ref[:, c : c + chunk].astype(BF16)) + mm(
                second, acc_ref[:, half + c : half + c + chunk].astype(BF16)
            )
            spread = spread.astype(BF16)
            for k in range(n):
                blocks[k][:, c : c + chunk] = spread[k * PIECE : (k + 1) * PIECE]


def expert(arrived, back, weights):
    n = len(arrived)
    slots = n * CAP
    hidden, width = weights.shape[1:]
    tile = 256
    half = width // FOLD
    outs = pl.pallas_call(
        lambda *refs: expert_kernel(n, slots, *refs),
        out_shape=[jax.ShapeDtypeStruct((slots // 2, width), BF16)] * 2
        + [jax.ShapeDtypeStruct((PIECE, half), BF16)] * n,
        grid=(hidden // tile,),
        in_specs=[whole(b.shape) for b in arrived]
        + [
            pl.BlockSpec((slots, tile), lambda i: (0, i)),
            pl.BlockSpec((2, tile, width), lambda i: (0, i, 0)),
        ],
        out_specs=[whole((slots // 2, width))] * 2 + [whole((PIECE, half))] * n,
        scratch_shapes=[pltpu.VMEM((slots, width), F32), pltpu.VMEM((slots, width), BF16)],
        compiler_params=params("arbitrary"),
        cost_estimate=pl.CostEstimate(flops=8 * 10**9, bytes_accessed=2 * 10**7, transcendentals=0),
        name="expert",
    )(*arrived, back, weights)
    return outs[:2], list(outs[2:])


def grads_kernel(count, share, dp_ref, *refs):
    row_parts, grad_parts = refs[:count], refs[count : 2 * count]
    weights, out_ref, rows_ref, grads_ref, w_ref, side_ref, sems = refs[2 * count :]
    part = row_parts[0].shape[0]
    chunk = out_ref.shape[2]

    @pl.when(pl.program_id(0) == 0)
    def _():
        first = pl.multiple_of(dp_ref[0] * share, 32)
        copies = []
        for i in range(3):
            source = weights.at[i, pl.ds(first, share)]
            copies.append(pltpu.make_async_copy(source, w_ref.at[i], sems.at[2 * count + i]))
        late = [copies.pop()]
        for i in range(count):
            at = pl.ds(i * part, part)
            copies.append(pltpu.make_async_copy(row_parts[i], rows_ref.at[at], sems.at[i]))
            late.append(pltpu.make_async_copy(grad_parts[i], grads_ref.at[at], sems.at[count + i]))
        for copy in copies + late:
            copy.start()
        for copy in copies:
            copy.wait()
        rows = rows_ref[...]
        gate_in = mm_t(rows, w_ref[0])
        up_in = mm_t(rows, w_ref[1])
        for copy in late:
            copy.wait()
        back = mm_t(grads_ref[...], w_ref[2])
        for i, side in enumerate(gated(gate_in, up_in, back)):
            side_ref[i] = side

    at = pl.ds(pl.multiple_of(pl.program_id(0) * chunk, chunk), chunk)
    out_ref[0] = t_mm(side_ref[0], rows_ref[:, at]).astype(BF16)
    out_ref[1] = t_mm(side_ref[1], rows_ref[:, at]).astype(BF16)
    out_ref[2] = t_mm(side_ref[2], grads_ref[:, at]).astype(BF16)


def expert_gradients(dp_index, row_parts, grad_parts, weights, share):
    count = len(row_parts)
    width = weights.shape[2]
    slots = row_parts[0].shape[0]
    total = count * slots
    chunk = width // 4
    anywhere = pl.BlockSpec(memory_space=pl.ANY)
    return pl.pallas_call(
        lambda *refs: grads_kernel(count, share, *refs),
        out_shape=jax.ShapeDtypeStruct((3, share, width), BF16),
        grid=(width // chunk,),
        in_specs=[SMEM_SPEC] + [anywhere] * (2 * count + 1),
        out_specs=pl.BlockSpec((3, share, chunk), lambda i: (0, 0, i)),
        scratch_shapes=[
            pltpu.VMEM((total, width), BF16),
            pltpu.VMEM((total, width), BF16),
            pltpu.VMEM((3, share, width), BF16),
            pltpu.VMEM((3, total, share), BF16),
            pltpu.SemaphoreType.DMA((2 * count + 3,)),
        ],
        compiler_params=params("arbitrary"),
        cost_estimate=pl.CostEstimate(flops=10**10, bytes_accessed=15 * 10**6, transcendentals=0),
        name="grads",
    )(dp_index, *row_parts, *grad_parts, weights)


def backward_kernel(n, rows, width, *refs):
    back_refs = refs[:n]
    pick_ref, up_ref, mixed_ref, gain_ref, factor_ref, q_ref, inv_ref, exp_ref, va_ref, kt_ref = refs[n : n + 10]
    dq_ref, near_ref, far_ref = refs[n + 10 : n + 13]
    gm_ref, ig_ref, dk_ref, dv_ref = refs[n + 13 :]
    step = pl.program_id(0)
    per_step = STEP_HEADS * HEAD_SIZE
    per_group = HEADS_PER_GROUP // STEP_HEADS
    chunks = width // per_step
    g = step // per_group

    @pl.when(step == 0)
    def _():
        half_chunks = chunks // FOLD
        total = jnp.zeros((rows, 1), F32)
        for i in range(chunks):
            f, c = i // half_chunks, (i % half_chunks) * per_step
            stacked = jnp.concatenate([b[:, c : c + per_step] for b in back_refs], axis=0)
            grad = t_mm(pick_ref[f], stacked) * gain_ref[:, i * per_step : (i + 1) * per_step]
            ig_ref[i] = grad
            mixed = mixed_ref[:, i * per_step : (i + 1) * per_step].astype(F32)
            total = total + jnp.sum(grad * mixed, axis=1, keepdims=True)
        factor = factor_ref[:, :1]
        pull = factor * factor * factor * (total / width)
        for i in range(chunks):
            mixed = mixed_ref[:, i * per_step : (i + 1) * per_step].astype(F32)
            up = up_ref[:, i * per_step : (i + 1) * per_step].astype(F32)
            gm_ref[i] = (up + (factor * ig_ref[i] - mixed * pull)).astype(BF16)

    @pl.when(step % per_group == 0)
    def _():
        dk_ref[...] = jnp.zeros_like(dk_ref)
        dv_ref[...] = jnp.zeros_like(dv_ref)

    col = pl.multiple_of(step * per_step, per_step)
    grad_all = gm_ref[step].astype(F32) * inv_ref[...]
    grad_b = grad_all.astype(BF16)
    prod = (grad_b.astype(F32) * mixed_ref[:, pl.ds(col, per_step)].astype(F32)).astype(BF16)

    def stack(x, p):
        at = p * 2 * HEAD_SIZE
        return jnp.concatenate([x[:, at : at + HEAD_SIZE], x[:, at + HEAD_SIZE : at + 2 * HEAD_SIZE]], axis=0)

    def push(p):
        return mm_t(va_ref[g], jnp.concatenate([stack(grad_b, p), stack(prod, p)], axis=1))

    ahead = push(0)
    for p in range(STEP_HEADS // 2):
        at = p * 2 * HEAD_SIZE
        gs = stack(grad_b, p)
        pushed = ahead
        if p + 1 < STEP_HEADS // 2:
            ahead = push(p + 1)
        exps = exp_ref[p]
        slopes = (exps.astype(F32) * pushed).astype(BF16)
        qs = jnp.concatenate([q_ref[:, at : at + HEAD_SIZE], q_ref[:, at + HEAD_SIZE : at + 2 * HEAD_SIZE]], axis=0)
        dk_ref[...] += mm(slopes, qs)
        dv_ref[...] += mm(exps, gs)
        dq = mm(kt_ref[g], slopes) * SCALE
        for i in range(2):
            cols = slice(at + i * HEAD_SIZE, at + (i + 1) * HEAD_SIZE)
            dq_ref[:, cols] = dq[:, i * rows : (i + 1) * rows].T.astype(BF16)

    groups = va_ref.shape[0]
    for gg in range(groups):

        @pl.when(step == (gg + 1) * per_group - 1)
        def _():
            for b in range(n):
                at = slice(b * rows, (b + 1) * rows)
                kcol = slice(gg * HEAD_SIZE, (gg + 1) * HEAD_SIZE)
                vcol = slice((groups + gg) * HEAD_SIZE, (groups + gg + 1) * HEAD_SIZE)
                if b % 2 == 0:
                    near_ref[b // 2, :, kcol] = dk_ref[at] * SCALE
                    near_ref[b // 2, :, vcol] = dv_ref[at]
                else:
                    far_ref[b // 2, :, kcol] = (dk_ref[at] * SCALE).astype(BF16)
                    far_ref[b // 2, :, vcol] = dv_ref[at].astype(BF16)


def backward(back, pick, upstream, gain, query, fwd):
    _, va, kt, _, exps, inv, mixed, factor = fwd
    n = len(back)
    rows, width = query.shape
    groups, total = va.shape[:2]
    per_step = STEP_HEADS * HEAD_SIZE
    steps = width // per_step
    column = pl.BlockSpec((rows, per_step), lambda i: (0, i))
    kv_width = 2 * groups * HEAD_SIZE
    return pl.pallas_call(
        lambda *refs: backward_kernel(n, rows, width, *refs),
        out_shape=[
            jax.ShapeDtypeStruct((rows, width), BF16),
            jax.ShapeDtypeStruct((n // 2, rows, kv_width), F32),
            jax.ShapeDtypeStruct((n // 2, rows, kv_width), BF16),
        ],
        grid=(steps,),
        in_specs=[whole(back[0].shape)] * n
        + [whole(pick.shape), whole(upstream.shape), whole(mixed.shape), whole(gain.shape), whole(factor.shape)]
        + [
            column,
            column,
            pl.BlockSpec((STEP_HEADS // 2, total, 2 * rows), lambda i: (i, 0, 0)),
            whole(va.shape),
            whole(kt.shape),
        ],
        out_specs=[column, whole((n // 2, rows, kv_width)), whole((n // 2, rows, kv_width))],
        scratch_shapes=[
            pltpu.VMEM((steps, rows, per_step), BF16),
            pltpu.VMEM((steps, rows, per_step), F32),
            pltpu.VMEM((total, HEAD_SIZE), F32),
            pltpu.VMEM((total, HEAD_SIZE), F32),
        ],
        compiler_params=params("arbitrary"),
        cost_estimate=pl.CostEstimate(flops=2 * 10**10, bytes_accessed=2 * 10**7, transcendentals=0),
        name="backward",
    )(*back, pick, upstream, mixed, gain, factor, query, inv, exps, va, kt)


def shift(x, axis, k):
    n = lax.axis_size(axis)
    return lax.ppermute(x, axis, [(i, (i + k) % n) for i in range(n)])


def flip(x, axis, bit):
    n = lax.axis_size(axis)
    return lax.ppermute(x, axis, [(i, i ^ bit) for i in range(n)])


def exchange(blocks, sign):
    n = len(blocks)
    got = [blocks[0]] + [None] * (n - 1)
    chips = n // 2
    for b in sorted(range(1, n), key=lambda b: -min(b // 2, chips - b // 2)):
        got[b] = lax.ppermute(blocks[b], "ctx", [(i, peer_of(i, b, n, sign)) for i in range(n)])
    return got


def gather_docs(parts):
    n = lax.axis_size("dp")
    bits = [1 << b for b in range(n.bit_length() - 1)]
    got = []
    for part, order in zip(parts, (bits, bits[::-1])):
        pieces = [part]
        for bit in order:
            moved = []
            for piece in pieces:
                moved.append(flip(piece, "dp", bit))
            pieces += moved
        got += pieces
    return got


def per_device(
    query,
    key,
    value,
    span_order,
    expert_ids,
    expert_gates,
    trainable,
    norm_gain,
    upstream,
    expert_weights,
):
    n = lax.axis_size("ctx")
    chips = n // 2
    me = lax.axis_index("ctx").astype(jnp.int32).reshape(1)
    dp_index = lax.axis_index("dp").astype(jnp.int32).reshape(1)
    weights = expert_weights[0].transpose(1, 0, 2)
    gain = norm_gain[None, :]
    grad_out = upstream[0]

    kv = jnp.concatenate([key[0], value[0]], axis=1)
    arrived = [kv] + [shift(kv, "ctx", 2 * m) for m in range(1, chips)]
    kv_blocks = []
    for block in arrived:
        kv_blocks += [block, flip(block, "ctx", 1)]

    pick, grad_blocks = route(me, trainable, expert_ids[0].T, expert_gates[0].T, grad_out)
    pairs = [shift(grad_blocks[m + 1], "ctx", 2 * m) for m in range(1, chips)]
    grad_blocks = [grad_blocks[0], flip(grad_blocks[1], "ctx", 1)]
    for pair in pairs:
        grad_blocks += [pair, flip(pair, "ctx", 1)]
    *weighted, back_rows = early(grad_blocks, weights)
    all_weighted = gather_docs(weighted)

    fwd, row_blocks = forward(me, span_order, kv_blocks, query[0], pick, gain)
    row_blocks = exchange(row_blocks, 1)
    routed, returned = expert(row_blocks, back_rows, weights)
    all_routed = gather_docs(routed)
    back = exchange(returned, -1)
    share = weights.shape[1] // lax.axis_size("dp")
    expert_grads = expert_gradients(dp_index, all_routed, all_weighted, weights, share)
    d_query, near, far = backward(back, pick, grad_out, gain, query[0], fwd)

    far = flip(far, "ctx", 1)
    met = near + far.astype(F32)
    total = met[0]
    sent = met.astype(BF16)
    landed = [shift(sent[m], "ctx", -2 * m) for m in range(1, chips)]
    for block in landed:
        total = total + block.astype(F32)
    split = key.shape[2]
    return (
        d_query[None],
        total[:, :split].astype(BF16)[None],
        total[:, split:].astype(BF16)[None],
        expert_grads.transpose(1, 0, 2)[None],
    )


def solution(mesh):
    in_specs = (
        P("dp", "ctx", None),
        P("dp", "ctx", None),
        P("dp", "ctx", None),
        P("dp", None),
        P("dp", "ctx", None),
        P("dp", "ctx", None),
        P(),
        P(),
        P("dp", "ctx", None),
        P("ctx", None, None, None),
    )
    out_specs = (
        P("dp", "ctx", None),
        P("dp", "ctx", None),
        P("dp", "ctx", None),
        P("ctx", "dp", None, None),
    )

    return jax.shard_map(per_device, mesh=mesh, in_specs=in_specs, out_specs=out_specs, check_vma=False)
```

```python
import jax
import jax.numpy as jnp
from jax import lax
from jax.experimental import pallas as pl
from jax.experimental.pallas import tpu as pltpu
from jax.sharding import PartitionSpec as P


HEADS_PER_GROUP = 16
HEAD_SIZE = 128
CAP = 12
EPSILON = 1e-06
MASK_FILLER = -1e30
SCALE = HEAD_SIZE ** (-0.5)
LOG2E = 1.4426950408889634
FOLD = 2
PIECE = FOLD * CAP
STEP_HEADS = 8
VMEM_BYTES = 67043328
F32 = jnp.float32
BF16 = jnp.bfloat16


def mm(a, b):
    return lax.dot_general(a, b, (((1,), (0,)), ((), ())), preferred_element_type=F32)


def mm_t(a, b):
    return lax.dot_general(a, b, (((1,), (1,)), ((), ())), preferred_element_type=F32)


def t_mm(a, b):
    return lax.dot_general(a, b, (((0,), (0,)), ((), ())), preferred_element_type=F32)


def iota(shape, dim):
    return lax.broadcasted_iota(jnp.int32, shape, dim)


def params(*semantics):
    if semantics:
        return pltpu.CompilerParams(dimension_semantics=semantics, vmem_limit_bytes=VMEM_BYTES)
    return pltpu.CompilerParams(vmem_limit_bytes=VMEM_BYTES)


def whole(shape):
    return pl.BlockSpec(shape, lambda *_: (0,) * len(shape))


SMEM_SPEC = pl.BlockSpec(memory_space=pltpu.SMEM)


def peer_of(me, b, n, sign):
    core = me % 2
    chip = (me // 2 + sign * (b // 2) + n // 2) % (n // 2)
    return 2 * chip + (core if b % 2 == 0 else 1 - core)


def route_kernel(n, rows, width, me_ref, train_ref, ids_ref, gates_ref, up_ref, *outs):
    pick_ref, blocks = outs[0], outs[1:]
    ids = ids_ref[...]
    gates = gates_ref[...]
    me = me_ref[0]
    row_n = iota((n, rows), 0)
    hits = jnp.zeros((n, rows), F32)
    level = jnp.zeros((n, rows), F32)
    for k in range(n):
        same = ids == train_ref[peer_of(me, k, n, 1)]
        hit = jnp.sum(same.astype(F32), axis=0, keepdims=True)
        gate = jnp.sum(jnp.where(same, gates, 0.0), axis=0, keepdims=True)
        hits = jnp.where(row_n == k, hit, hits)
        level = jnp.where(row_n == k, gate, level)
    before = (iota((rows, rows), 0) < iota((rows, rows), 1)).astype(BF16)
    rank = mm(hits.astype(BF16), before)
    place = jnp.where(hits > 0.5, rank, 1e4)
    sub = iota((PIECE, rows), 0)
    slot = jnp.where(sub >= CAP, sub - CAP, sub).astype(F32)
    firsts, seconds, scales = [], [], []
    for k in range(n):
        chosen = place[k : k + 1, :] == slot
        firsts.append(jnp.where(chosen & (sub < CAP), 1.0, 0.0))
        seconds.append(jnp.where(chosen & (sub >= CAP), 1.0, 0.0))
        scales.append(jnp.sum(jnp.where(chosen, level[k : k + 1, :], 0.0), axis=1, keepdims=True))
    first = jnp.concatenate(firsts, axis=0).astype(BF16)
    second = jnp.concatenate(seconds, axis=0).astype(BF16)
    scale = jnp.concatenate(scales, axis=0)
    pick_ref[0] = first
    pick_ref[1] = second
    half = width // FOLD
    chunk = min(512, half)
    for c in range(0, half, chunk):
        picked = mm(first, up_ref[:, c : c + chunk]) + mm(second, up_ref[:, half + c : half + c + chunk])
        picked = (picked * scale).astype(BF16)
        for k in range(2):
            blocks[k][:, c : c + chunk] = picked[k * PIECE : (k + 1) * PIECE]
        for m in range(1, n // 2):
            blocks[m + 1][:, c : c + chunk] = picked[2 * m * PIECE : 2 * (m + 1) * PIECE]


def route(me, trainable, ids, gates, upstream):
    n = trainable.shape[0]
    rows, width = upstream.shape
    half = width // FOLD
    out_shape = [jax.ShapeDtypeStruct((2, n * PIECE, rows), BF16)] + [
        jax.ShapeDtypeStruct((PIECE if m < 2 else 2 * PIECE, half), BF16) for m in range(n // 2 + 1)
    ]
    outs = pl.pallas_call(
        lambda *refs: route_kernel(n, rows, width, *refs),
        out_shape=out_shape,
        in_specs=[SMEM_SPEC, SMEM_SPEC] + [pl.BlockSpec(memory_space=pltpu.VMEM)] * 3,
        compiler_params=params(),
        cost_estimate=pl.CostEstimate(flops=4 * 10**9, bytes_accessed=2 * 10**6, transcendentals=0),
        name="route",
    )(me, trainable, ids, gates, upstream)
    return outs[0], list(outs[1:])


def unfold(pieces, out_ref):
    n = len(pieces)
    slots, width = out_ref.shape
    half = width // FOLD
    r = iota((slots, n * PIECE), 0)
    s = iota((slots, n * PIECE), 1)
    start = r
    for k in range(1, n):
        start = start + jnp.where(r >= k * CAP, PIECE - CAP, 0)
    chunk = min(512, half)
    for f in range(FOLD):
        select = (s == start + f * CAP).astype(BF16)
        for c in range(0, half, chunk):
            stacked = jnp.concatenate([ref[at : at + PIECE, c : c + chunk] for ref, at in pieces], axis=0)
            at = f * half + c
            out_ref[:, at : at + chunk] = mm(select, stacked).astype(BF16)


def forward_kernel(n, rows, width, me_ref, span_ref, *refs):
    kv_refs = refs[:n]
    q_ref, pick_ref, gain_ref = refs[n : n + 3]
    ka_ref, va_ref, kt_ref, vt_ref, exp_ref, inv_ref, mixed_ref, factor_ref = refs[n + 3 : n + 11]
    blocks = refs[n + 11 : n + 11 + n]
    b_ref, all_ref = refs[n + 11 + n :]
    step = pl.program_id(0)
    half_rows = rows // 2
    per_step = STEP_HEADS * HEAD_SIZE
    groups = ka_ref.shape[0]

    @pl.when(step == 0)
    def _():
        me = me_ref[0]
        lane = iota((rows, rows), 1)
        sub = iota((rows, rows), 0)
        lane_half = (lane >= half_rows).astype(jnp.int32)
        sub_half = (sub >= half_rows).astype(jnp.int32)
        lane_in = lane - lane_half * half_rows
        sub_in = sub - sub_half * half_rows
        b_ref[...] = jnp.where((lane_half == sub_half) & (lane_in >= sub_in), MASK_FILLER, 0.0).astype(BF16)
        mine0 = span_ref[0, 2 * me]
        mine1 = span_ref[0, 2 * me + 1]
        lane_span = jnp.where(lane_half == 0, mine0, mine1)
        for b in range(n):
            source = peer_of(me, b, n, -1)
            sub_span = jnp.where(sub_half == 0, span_ref[0, 2 * source], span_ref[0, 2 * source + 1])
            hot = ((sub_span == lane_span) & (lane_in == sub_in - 1)) | (
                (sub_span > lane_span) & (lane_in == half_rows - 1)
            )
            hot = jnp.where(hot, 1.0, 0.0).astype(BF16)
            kv = kv_refs[b][...]
            at = slice(b * rows, (b + 1) * rows)
            for g in range(groups):
                key = kv[:, g * HEAD_SIZE : (g + 1) * HEAD_SIZE]
                value = kv[:, (groups + g) * HEAD_SIZE : (groups + g + 1) * HEAD_SIZE]
                ka_ref[g, at, :HEAD_SIZE] = key
                ka_ref[g, at, HEAD_SIZE:] = hot
                va_ref[g, at, :HEAD_SIZE] = value
                va_ref[g, at, HEAD_SIZE:] = jnp.full((rows, HEAD_SIZE), -1.0, BF16)
                kt_ref[g, :, at] = key.T
                vt_ref[g, :HEAD_SIZE, at] = value.T
                vt_ref[g, HEAD_SIZE:, at] = jnp.ones((16, rows), BF16)

    g = step // (HEADS_PER_GROUP // STEP_HEADS)
    b = b_ref[...]

    def paired(p):
        at = p * 2 * HEAD_SIZE
        q0 = q_ref[:, at : at + HEAD_SIZE]
        q1 = q_ref[:, at + HEAD_SIZE : at + 2 * HEAD_SIZE]
        return jnp.concatenate(
            [jnp.concatenate([q0, b], axis=1), jnp.concatenate([q1, b], axis=1)], axis=0
        )

    ahead = mm_t(ka_ref[g], paired(0))
    for p in range(STEP_HEADS // 2):
        at = p * 2 * HEAD_SIZE
        scores = ahead
        if p + 1 < STEP_HEADS // 2:
            ahead = mm_t(ka_ref[g], paired(p + 1))
        peak = jnp.max(scores, axis=0, keepdims=True)
        exps = jnp.exp2((scores - peak) * (SCALE * LOG2E)).astype(BF16)
        exp_ref[p] = exps
        out = mm(vt_ref[g], exps)
        inv = 1.0 / out[HEAD_SIZE : HEAD_SIZE + 1, :]
        normal = out[:HEAD_SIZE, :] * inv
        inv_full = jnp.broadcast_to(inv, (rows, 2 * rows))
        for i in range(2):
            cols = slice(at + i * HEAD_SIZE, at + (i + 1) * HEAD_SIZE)
            head = normal[:, i * rows : (i + 1) * rows].T.astype(BF16)
            mixed_ref[:, cols] = head
            all_ref[step, :, cols] = head
            inv_ref[:, cols] = inv_full[:, i * rows : (i + 1) * rows].T

    @pl.when(step == pl.num_programs(0) - 1)
    def _():
        steps = width // per_step
        square = jnp.zeros((rows, 1), F32)
        for i in range(steps):
            part = all_ref[i].astype(F32)
            square = square + jnp.sum(part * part, axis=1, keepdims=True)
        factor = lax.rsqrt(square / width + EPSILON)
        factor_ref[...] = jnp.broadcast_to(factor, (rows, 128))

        def normed(i):
            gain = gain_ref[:, i * per_step : (i + 1) * per_step]
            return (all_ref[i].astype(F32) * factor * gain).astype(BF16)

        for i in range(steps // FOLD):
            picked = mm(pick_ref[0], normed(i)) + mm(pick_ref[1], normed(steps // FOLD + i))
            picked = picked.astype(BF16)
            for k in range(n):
                blocks[k][:, i * per_step : (i + 1) * per_step] = picked[k * PIECE : (k + 1) * PIECE]


def forward(me, span, kv_blocks, query, pick, gain):
    n = len(kv_blocks)
    rows, width = query.shape
    groups = kv_blocks[0].shape[1] // (2 * HEAD_SIZE)
    total = n * rows
    per_step = STEP_HEADS * HEAD_SIZE
    steps = width // per_step
    half = width // FOLD
    pairs = width // (2 * HEAD_SIZE)
    out_shape = [
        jax.ShapeDtypeStruct((groups, total, 2 * HEAD_SIZE), BF16),
        jax.ShapeDtypeStruct((groups, total, 2 * HEAD_SIZE), BF16),
        jax.ShapeDtypeStruct((groups, HEAD_SIZE, total), BF16),
        jax.ShapeDtypeStruct((groups, HEAD_SIZE + 16, total), BF16),
        jax.ShapeDtypeStruct((pairs, total, 2 * rows), BF16),
        jax.ShapeDtypeStruct((rows, width), F32),
        jax.ShapeDtypeStruct((rows, width), BF16),
        jax.ShapeDtypeStruct((rows, 128), F32),
    ] + [jax.ShapeDtypeStruct((PIECE, half), BF16) for _ in range(n)]
    column = pl.BlockSpec((rows, per_step), lambda i: (0, i))
    out_specs = [whole(s.shape) for s in out_shape]
    out_specs[4] = pl.BlockSpec((STEP_HEADS // 2, total, 2 * rows), lambda i: (i, 0, 0))
    out_specs[5] = column
    out_specs[6] = column
    outs = pl.pallas_call(
        lambda *refs: forward_kernel(n, rows, width, *refs),
        out_shape=out_shape,
        grid=(steps,),
        in_specs=[SMEM_SPEC, SMEM_SPEC]
        + [whole(kv_blocks[0].shape)] * n
        + [column, whole(pick.shape), whole(gain.shape)],
        out_specs=out_specs,
        scratch_shapes=[pltpu.VMEM((rows, rows), BF16), pltpu.VMEM((steps, rows, per_step), BF16)],
        compiler_params=params("arbitrary"),
        cost_estimate=pl.CostEstimate(flops=10**10, bytes_accessed=2 * 10**7, transcendentals=4 * 10**6),
        name="forward",
    )(me, span, *kv_blocks, query, pick, gain)
    return outs[:8], list(outs[8:])


def gated(gate_in, up_in, back):
    sigma = 1.0 / (1.0 + jnp.exp(-gate_in))
    act = gate_in * sigma
    grad_gate = (back * up_in * sigma * (1.0 + gate_in * (1.0 - sigma))).astype(BF16)
    grad_up = (back * act).astype(BF16)
    product = (act * up_in).astype(BF16)
    return grad_gate, grad_up, product


def split_rows(rows_ref, halves):
    part = halves[0].shape[0]
    for i, half in enumerate(halves):
        half[...] = rows_ref[i * part : (i + 1) * part]


def early_kernel(n, *refs):
    blocks, (weights, *halves, back_ref, rows_ref) = refs[:n], refs[n:]

    @pl.when(pl.program_id(0) == 0)
    def _():
        unfold([(ref, PIECE if b > 2 and b % 2 else 0) for b, ref in enumerate(blocks)], rows_ref)
        split_rows(rows_ref, halves)

    back_ref[...] = mm_t(rows_ref[...], weights[0])


def early(blocks, weights):
    n = len(blocks)
    hidden, width = weights.shape[1:]
    slots = n * CAP
    tile = 256
    return pl.pallas_call(
        lambda *refs: early_kernel(n, *refs),
        out_shape=[jax.ShapeDtypeStruct((slots // 2, width), BF16)] * 2
        + [jax.ShapeDtypeStruct((slots, hidden), F32)],
        grid=(hidden // tile,),
        scratch_shapes=[pltpu.VMEM((slots, width), BF16)],
        in_specs=[whole(b.shape) for b in blocks] + [pl.BlockSpec((1, tile, width), lambda i: (2, i, 0))],
        out_specs=[whole((slots // 2, width))] * 2 + [pl.BlockSpec((slots, tile), lambda i: (0, i))],
        compiler_params=params("arbitrary"),
        cost_estimate=pl.CostEstimate(flops=2 * 10**9, bytes_accessed=7 * 10**6, transcendentals=0),
        name="early",
    )(*blocks, weights)


def expert_kernel(n, slots, *refs):
    arrived, (back_ref, weights, *halves) = refs[:n], refs[n : n + 4]
    blocks, (acc_ref, routed_ref) = refs[n + 4 : -2], refs[-2:]
    step = pl.program_id(0)
    width = acc_ref.shape[1]

    @pl.when(step == 0)
    def _():
        unfold([(ref, 0) for ref in arrived], routed_ref)
        split_rows(routed_ref, halves)

    routed = routed_ref[...]
    gate_in = mm_t(routed, weights[0])
    up_in = mm_t(routed, weights[1])
    grad_gate, grad_up, _ = gated(gate_in, up_in, back_ref[...])
    got = mm(grad_gate, weights[0]) + mm(grad_up, weights[1])

    @pl.when(step == 0)
    def _():
        acc_ref[...] = got

    @pl.when(step > 0)
    def _():
        acc_ref[...] += got

    @pl.when(step == pl.num_programs(0) - 1)
    def _():
        half = width // FOLD
        r = iota((n * PIECE, slots), 1)
        s = iota((n * PIECE, slots), 0)
        start = r
        for k in range(1, n):
            start = start + jnp.where(r >= k * CAP, PIECE - CAP, 0)
        first = (s == start).astype(BF16)
        second = (s == start + CAP).astype(BF16)
        chunk = min(512, half)
        for c in range(0, half, chunk):
            spread = mm(first, acc_ref[:, c : c + chunk].astype(BF16)) + mm(
                second, acc_ref[:, half + c : half + c + chunk].astype(BF16)
            )
            spread = spread.astype(BF16)
            for k in range(n):
                blocks[k][:, c : c + chunk] = spread[k * PIECE : (k + 1) * PIECE]


def expert(arrived, back, weights):
    n = len(arrived)
    slots = n * CAP
    hidden, width = weights.shape[1:]
    tile = 256
    half = width // FOLD
    outs = pl.pallas_call(
        lambda *refs: expert_kernel(n, slots, *refs),
        out_shape=[jax.ShapeDtypeStruct((slots // 2, width), BF16)] * 2
        + [jax.ShapeDtypeStruct((PIECE, half), BF16)] * n,
        grid=(hidden // tile,),
        in_specs=[whole(b.shape) for b in arrived]
        + [
            pl.BlockSpec((slots, tile), lambda i: (0, i)),
            pl.BlockSpec((2, tile, width), lambda i: (0, i, 0)),
        ],
        out_specs=[whole((slots // 2, width))] * 2 + [whole((PIECE, half))] * n,
        scratch_shapes=[pltpu.VMEM((slots, width), F32), pltpu.VMEM((slots, width), BF16)],
        compiler_params=params("arbitrary"),
        cost_estimate=pl.CostEstimate(flops=8 * 10**9, bytes_accessed=2 * 10**7, transcendentals=0),
        name="expert",
    )(*arrived, back, weights)
    return outs[:2], list(outs[2:])


def grads_kernel(count, share, dp_ref, *refs):
    row_parts, grad_parts = refs[:count], refs[count : 2 * count]
    weights, out_ref, rows_ref, grads_ref, w_ref, side_ref, sems = refs[2 * count :]
    part = row_parts[0].shape[0]
    chunk = out_ref.shape[2]

    @pl.when(pl.program_id(0) == 0)
    def _():
        first = pl.multiple_of(dp_ref[0] * share, 32)
        copies = []
        for i in range(3):
            source = weights.at[i, pl.ds(first, share)]
            copies.append(pltpu.make_async_copy(source, w_ref.at[i], sems.at[2 * count + i]))
        late = [copies.pop()]
        for i in range(count):
            at = pl.ds(i * part, part)
            copies.append(pltpu.make_async_copy(row_parts[i], rows_ref.at[at], sems.at[i]))
            late.append(pltpu.make_async_copy(grad_parts[i], grads_ref.at[at], sems.at[count + i]))
        for copy in copies + late:
            copy.start()
        for copy in copies:
            copy.wait()
        rows = rows_ref[...]
        gate_in = mm_t(rows, w_ref[0])
        up_in = mm_t(rows, w_ref[1])
        for copy in late:
            copy.wait()
        back = mm_t(grads_ref[...], w_ref[2])
        for i, side in enumerate(gated(gate_in, up_in, back)):
            side_ref[i] = side

    at = pl.ds(pl.multiple_of(pl.program_id(0) * chunk, chunk), chunk)
    out_ref[0] = t_mm(side_ref[0], rows_ref[:, at]).astype(BF16)
    out_ref[1] = t_mm(side_ref[1], rows_ref[:, at]).astype(BF16)
    out_ref[2] = t_mm(side_ref[2], grads_ref[:, at]).astype(BF16)


def expert_gradients(dp_index, row_parts, grad_parts, weights, share):
    count = len(row_parts)
    width = weights.shape[2]
    slots = row_parts[0].shape[0]
    total = count * slots
    chunk = width // 4
    anywhere = pl.BlockSpec(memory_space=pl.ANY)
    return pl.pallas_call(
        lambda *refs: grads_kernel(count, share, *refs),
        out_shape=jax.ShapeDtypeStruct((3, share, width), BF16),
        grid=(width // chunk,),
        in_specs=[SMEM_SPEC] + [anywhere] * (2 * count + 1),
        out_specs=pl.BlockSpec((3, share, chunk), lambda i: (0, 0, i)),
        scratch_shapes=[
            pltpu.VMEM((total, width), BF16),
            pltpu.VMEM((total, width), BF16),
            pltpu.VMEM((3, share, width), BF16),
            pltpu.VMEM((3, total, share), BF16),
            pltpu.SemaphoreType.DMA((2 * count + 3,)),
        ],
        compiler_params=params("arbitrary"),
        cost_estimate=pl.CostEstimate(flops=10**10, bytes_accessed=15 * 10**6, transcendentals=0),
        name="grads",
    )(dp_index, *row_parts, *grad_parts, weights)


def backward_kernel(n, rows, width, *refs):
    back_refs = refs[:n]
    pick_ref, up_ref, mixed_ref, gain_ref, factor_ref, q_ref, inv_ref, exp_ref, va_ref, kt_ref = refs[n : n + 10]
    dq_ref, near_ref, far_ref = refs[n + 10 : n + 13]
    gm_ref, ig_ref, dk_ref, dv_ref = refs[n + 13 :]
    step = pl.program_id(0)
    per_step = STEP_HEADS * HEAD_SIZE
    per_group = HEADS_PER_GROUP // STEP_HEADS
    chunks = width // per_step
    g = step // per_group

    @pl.when(step == 0)
    def _():
        half_chunks = chunks // FOLD
        total = jnp.zeros((rows, 1), F32)
        for i in range(chunks):
            f, c = i // half_chunks, (i % half_chunks) * per_step
            stacked = jnp.concatenate([b[:, c : c + per_step] for b in back_refs], axis=0)
            grad = t_mm(pick_ref[f], stacked) * gain_ref[:, i * per_step : (i + 1) * per_step]
            ig_ref[i] = grad
            mixed = mixed_ref[:, i * per_step : (i + 1) * per_step].astype(F32)
            total = total + jnp.sum(grad * mixed, axis=1, keepdims=True)
        factor = factor_ref[:, :1]
        pull = factor * factor * factor * (total / width)
        for i in range(chunks):
            mixed = mixed_ref[:, i * per_step : (i + 1) * per_step].astype(F32)
            up = up_ref[:, i * per_step : (i + 1) * per_step].astype(F32)
            gm_ref[i] = (up + (factor * ig_ref[i] - mixed * pull)).astype(BF16)

    @pl.when(step % per_group == 0)
    def _():
        dk_ref[...] = jnp.zeros_like(dk_ref)
        dv_ref[...] = jnp.zeros_like(dv_ref)

    col = pl.multiple_of(step * per_step, per_step)
    grad_all = gm_ref[step].astype(F32) * inv_ref[...]
    grad_b = grad_all.astype(BF16)
    prod = (grad_b.astype(F32) * mixed_ref[:, pl.ds(col, per_step)].astype(F32)).astype(BF16)

    def stack(x, p):
        at = p * 2 * HEAD_SIZE
        return jnp.concatenate([x[:, at : at + HEAD_SIZE], x[:, at + HEAD_SIZE : at + 2 * HEAD_SIZE]], axis=0)

    def push(p):
        return mm_t(va_ref[g], jnp.concatenate([stack(grad_b, p), stack(prod, p)], axis=1))

    ahead = push(0)
    for p in range(STEP_HEADS // 2):
        at = p * 2 * HEAD_SIZE
        gs = stack(grad_b, p)
        pushed = ahead
        if p + 1 < STEP_HEADS // 2:
            ahead = push(p + 1)
        exps = exp_ref[p]
        slopes = (exps.astype(F32) * pushed).astype(BF16)
        qs = jnp.concatenate([q_ref[:, at : at + HEAD_SIZE], q_ref[:, at + HEAD_SIZE : at + 2 * HEAD_SIZE]], axis=0)
        dk_ref[...] += mm(slopes, qs)
        dv_ref[...] += mm(exps, gs)
        dq = mm(kt_ref[g], slopes) * SCALE
        for i in range(2):
            cols = slice(at + i * HEAD_SIZE, at + (i + 1) * HEAD_SIZE)
            dq_ref[:, cols] = dq[:, i * rows : (i + 1) * rows].T.astype(BF16)

    groups = va_ref.shape[0]
    for gg in range(groups):

        @pl.when(step == (gg + 1) * per_group - 1)
        def _():
            for b in range(n):
                at = slice(b * rows, (b + 1) * rows)
                kcol = slice(gg * HEAD_SIZE, (gg + 1) * HEAD_SIZE)
                vcol = slice((groups + gg) * HEAD_SIZE, (groups + gg + 1) * HEAD_SIZE)
                if b % 2 == 0:
                    near_ref[b // 2, :, kcol] = dk_ref[at] * SCALE
                    near_ref[b // 2, :, vcol] = dv_ref[at]
                else:
                    far_ref[b // 2, :, kcol] = (dk_ref[at] * SCALE).astype(BF16)
                    far_ref[b // 2, :, vcol] = dv_ref[at].astype(BF16)


def backward(back, pick, upstream, gain, query, fwd):
    _, va, kt, _, exps, inv, mixed, factor = fwd
    n = len(back)
    rows, width = query.shape
    groups, total = va.shape[:2]
    per_step = STEP_HEADS * HEAD_SIZE
    steps = width // per_step
    column = pl.BlockSpec((rows, per_step), lambda i: (0, i))
    kv_width = 2 * groups * HEAD_SIZE
    return pl.pallas_call(
        lambda *refs: backward_kernel(n, rows, width, *refs),
        out_shape=[
            jax.ShapeDtypeStruct((rows, width), BF16),
            jax.ShapeDtypeStruct((n // 2, rows, kv_width), F32),
            jax.ShapeDtypeStruct((n // 2, rows, kv_width), BF16),
        ],
        grid=(steps,),
        in_specs=[whole(back[0].shape)] * n
        + [whole(pick.shape), whole(upstream.shape), whole(mixed.shape), whole(gain.shape), whole(factor.shape)]
        + [
            column,
            column,
            pl.BlockSpec((STEP_HEADS // 2, total, 2 * rows), lambda i: (i, 0, 0)),
            whole(va.shape),
            whole(kt.shape),
        ],
        out_specs=[column, whole((n // 2, rows, kv_width)), whole((n // 2, rows, kv_width))],
        scratch_shapes=[
            pltpu.VMEM((steps, rows, per_step), BF16),
            pltpu.VMEM((steps, rows, per_step), F32),
            pltpu.VMEM((total, HEAD_SIZE), F32),
            pltpu.VMEM((total, HEAD_SIZE), F32),
        ],
        compiler_params=params("arbitrary"),
        cost_estimate=pl.CostEstimate(flops=2 * 10**10, bytes_accessed=2 * 10**7, transcendentals=0),
        name="backward",
    )(*back, pick, upstream, mixed, gain, factor, query, inv, exps, va, kt)


def shift(x, axis, k):
    n = lax.axis_size(axis)
    return lax.ppermute(x, axis, [(i, (i + k) % n) for i in range(n)])


def flip(x, axis, bit):
    n = lax.axis_size(axis)
    return lax.ppermute(x, axis, [(i, i ^ bit) for i in range(n)])


def exchange(blocks, sign):
    n = len(blocks)
    got = [blocks[0]] + [None] * (n - 1)
    chips = n // 2
    for b in sorted(range(1, n), key=lambda b: -min(b // 2, chips - b // 2)):
        got[b] = lax.ppermute(blocks[b], "ctx", [(i, peer_of(i, b, n, sign)) for i in range(n)])
    return got


def gather_docs(parts):
    n = lax.axis_size("dp")
    bits = [1 << b for b in range(n.bit_length() - 1)]
    got = []
    for part, order in zip(parts, (bits, bits[::-1])):
        pieces = [part]
        for bit in order:
            moved = []
            for piece in pieces:
                moved.append(flip(piece, "dp", bit))
            pieces += moved
        got += pieces
    return got


def per_device(
    query,
    key,
    value,
    span_order,
    expert_ids,
    expert_gates,
    trainable,
    norm_gain,
    upstream,
    expert_weights,
):
    n = lax.axis_size("ctx")
    chips = n // 2
    me = lax.axis_index("ctx").astype(jnp.int32).reshape(1)
    dp_index = lax.axis_index("dp").astype(jnp.int32).reshape(1)
    weights = expert_weights[0].transpose(1, 0, 2)
    gain = norm_gain[None, :]
    grad_out = upstream[0]

    kv = jnp.concatenate([key[0], value[0]], axis=1)
    arrived = [kv] + [shift(kv, "ctx", 2 * m) for m in range(1, chips)]
    kv_blocks = []
    for block in arrived:
        kv_blocks += [block, flip(block, "ctx", 1)]

    pick, grad_blocks = route(me, trainable, expert_ids[0].T, expert_gates[0].T, grad_out)
    pairs = [shift(grad_blocks[m + 1], "ctx", 2 * m) for m in range(1, chips)]
    grad_blocks = [grad_blocks[0], flip(grad_blocks[1], "ctx", 1)]
    for pair in pairs:
        grad_blocks += [pair, flip(pair, "ctx", 1)]
    *weighted, back_rows = early(grad_blocks, weights)
    all_weighted = gather_docs(weighted)

    fwd, row_blocks = forward(me, span_order, kv_blocks, query[0], pick, gain)
    row_blocks = exchange(row_blocks, 1)
    routed, returned = expert(row_blocks, back_rows, weights)
    all_routed = gather_docs(routed)
    back = exchange(returned, -1)
    share = weights.shape[1] // lax.axis_size("dp")
    expert_grads = expert_gradients(dp_index, all_routed, all_weighted, weights, share)
    d_query, near, far = backward(back, pick, grad_out, gain, query[0], fwd)

    far = flip(far, "ctx", 1)
    met = near + far.astype(F32)
    total = met[0]
    sent = met.astype(BF16)
    landed = [shift(sent[m], "ctx", -2 * m) for m in range(1, chips)]
    for block in landed:
        total = total + block.astype(F32)
    split = key.shape[2]
    return (
        d_query[None],
        total[:, :split].astype(BF16)[None],
        total[:, split:].astype(BF16)[None],
        expert_grads.transpose(1, 0, 2)[None],
    )


def solution(mesh):
    in_specs = (
        P("dp", "ctx", None),
        P("dp", "ctx", None),
        P("dp", "ctx", None),
        P("dp", None),
        P("dp", "ctx", None),
        P("dp", "ctx", None),
        P(),
        P(),
        P("dp", "ctx", None),
        P("ctx", None, None, None),
    )
    out_specs = (
        P("dp", "ctx", None),
        P("dp", "ctx", None),
        P("dp", "ctx", None),
        P("ctx", "dp", None, None),
    )

    return jax.shard_map(per_device, mesh=mesh, in_specs=in_specs, out_specs=out_specs, check_vma=False)
```
